16 devices in a mesh: dp: 4 (over z, y), tp: 4 (over x, core).
Axes of the slice: x: 2, y: 2, z: 2, core: 2. Of those that a mesh axis runs over, the one named last changes fastest.
Arguments:
- x: bfloat16 [12288, 5120], P('dp'), parts along dimension 0
- lens: int32 [8], P('dp'), parts along dimension 0
- g1: bfloat16 [5120], replicated
- g2: bfloat16 [5120], replicated
- wq: bfloat16 [5120, 4096], P(None, 'tp')
- wk: bfloat16 [5120, 1024], replicated
- wv: bfloat16 [5120, 1024], replicated
- wo: bfloat16 [4096, 5120], P('tp')
- wg: bfloat16 [5120, 14336], P(None, 'tp')
- wu: bfloat16 [5120, 14336], P(None, 'tp')
- wd: bfloat16 [14336, 5120], P('tp')
Outputs:
- output 1: bfloat16 [12288, 5120], P('dp'), parts along dimension 0
- output 2: bfloat16 [8, 3072, 8, 128], P('dp', None, 'tp'), parts along dimension 0
- output 3: bfloat16 [8, 3072, 8, 128], P('dp', None, 'tp'), parts along dimension 0
There are 4 independent parts. The reference program is written for one: setup_inputs(seed, part) draws one part's arguments, and reference() takes and returns one part's arrays. A program takes and returns all parts, laid end to end along the dimension named above; an argument that names none is the same for every part.
All inputs are finite; a program needn't handle non-finite values.
Results may differ from the reference program's by a relative error of at most 0.0136576.
Values are sent between devices in bfloat16 or wider.
A program may use at most 1 GiB of HBM per device.

```python
import numpy as np
import jax
import jax.numpy as jnp
from jax import lax

D = 5120
HEADS = 32
KV_HEADS = 8
HEAD = 128
FF = 14336
T = 3072
KVR = 8

QB = min(T, 256)
EPS = 1e-5
BASE = 500000.0


def setup_inputs(seed: int = 0, part: int = 0) -> dict:
    key = jax.random.PRNGKey(seed)
    kp = jax.random.split(jax.random.fold_in(key, part), 4)
    kw = jax.random.split(jax.random.fold_in(key, 1000003), 9)
    kl = jax.random.split(jax.random.fold_in(jax.random.fold_in(key, 7), part), 2)
    t = jnp.arange(T, dtype=jnp.float32)
    freq = jnp.array([1.0, 2.0, 3.0, 5.0], dtype=jnp.float32)
    phase = jax.random.uniform(kp[0], (4,), jnp.float32, 0.0, 2.0 * np.pi)
    amp = 0.5 * jax.random.normal(kp[1], (4, D), jnp.float32)
    wave = jnp.cos(2.0 * np.pi * t[:, None] * freq[None, :] / T + phase[None, :])
    x = jnp.dot(wave, amp) + 0.6 * jax.random.normal(kp[2], (T, D), jnp.float32)
    s = jax.random.randint(kl[0], (), 1, T // 16 + 1, dtype=jnp.int32)
    l1 = jnp.where(jax.random.bernoulli(kl[1]), s, T - s).astype(jnp.int32)
    lens = jnp.stack([l1, T - l1]).astype(jnp.int32)

    def w(k, shape, fan_in, gain=1.0):
        return (gain * fan_in ** -0.5 * jax.random.normal(k, shape, jnp.float32)).astype(jnp.bfloat16)

    return dict(
        x=x.astype(jnp.bfloat16),
        lens=lens,
        g1=(1.0 + 0.2 * jax.random.normal(kw[0], (D,), jnp.float32)).astype(jnp.bfloat16),
        g2=(1.0 + 0.2 * jax.random.normal(kw[1], (D,), jnp.float32)).astype(jnp.bfloat16),
        wq=w(kw[2], (D, HEADS * HEAD), D),
        wk=w(kw[3], (D, KV_HEADS * HEAD), D),
        wv=w(kw[4], (D, KV_HEADS * HEAD), D),
        wo=w(kw[5], (HEADS * HEAD, D), HEADS * HEAD, 2.0),
        wg=w(kw[6], (D, FF), D),
        wu=w(kw[7], (D, FF), D),
        wd=w(kw[8], (FF, D), FF),
    )


def _mm(a, b):
    return jnp.dot(a, b, preferred_element_type=jnp.float32)


def _rms(x, g):
    xf = x.astype(jnp.float32)
    ms = jnp.mean(xf * xf, axis=-1, keepdims=True)
    return (xf * lax.rsqrt(ms + EPS) * g.astype(jnp.float32)).astype(jnp.bfloat16)


def _rope(x, pos):
    inv = BASE ** (-jnp.arange(0, HEAD, 2, dtype=jnp.float32) / HEAD)
    ang = pos.astype(jnp.float32)[:, None] * inv[None, :]
    c = jnp.cos(ang)[:, None, :]
    s = jnp.sin(ang)[:, None, :]
    x1 = x[..., : HEAD // 2]
    x2 = x[..., HEAD // 2 :]
    return jnp.concatenate([x1 * c - x2 * s, x2 * c + x1 * s], axis=-1)


def _attention(q, k, v, seg):
    rep = HEADS // KV_HEADS
    nb = T // QB
    rows = jnp.arange(T)
    qg = jnp.transpose(q.reshape(T, KV_HEADS, rep, HEAD), (1, 0, 2, 3)).astype(jnp.float32)
    kg = jnp.transpose(k, (1, 0, 2)).astype(jnp.float32)
    vg = jnp.transpose(v, (1, 0, 2)).astype(jnp.float32)

    def group(args):
        qh, kh, vh = args

        def block(args2):
            qq, i = args2
            rq = i * QB + jnp.arange(QB)
            s = jnp.einsum('qrd,kd->rqk', qq, kh) * (HEAD ** -0.5)
            mask = (rows[None, :] <= rq[:, None]) & (seg[None, :] == seg[rq][:, None])
            s = jnp.where(mask[None], s, -jnp.inf)
            pr = jax.nn.softmax(s, axis=-1).astype(jnp.bfloat16).astype(jnp.float32)
            return jnp.einsum('rqk,kd->qrd', pr, vh).astype(jnp.bfloat16)

        o = lax.map(block, (qh.reshape(nb, QB, rep, HEAD), jnp.arange(nb)))
        return o.reshape(T, rep, HEAD)

    o = lax.map(group, (qg, kg, vg))
    return jnp.transpose(o, (1, 0, 2, 3)).reshape(T, HEADS * HEAD)


def _cache(k, l1):
    rows = jnp.arange(T)
    z = jnp.zeros((), k.dtype)
    c1 = jnp.where((rows < l1)[:, None, None], k, z)
    c2 = jnp.where((rows < T - l1)[:, None, None], jnp.take(k, (rows + l1) % T, axis=0), z)
    return jnp.stack([c1, c2])


def reference(x, lens, g1, g2, wq, wk, wv, wo, wg, wu, wd):
    l1 = lens[0]
    rows = jnp.arange(T)
    seg = (rows >= l1).astype(jnp.int32)
    pos = jnp.where(seg == 1, rows - l1, rows)
    a = _rms(x, g1)
    q = _rope(_mm(a, wq).reshape(T, HEADS, HEAD), pos).astype(jnp.bfloat16)
    k = _rope(_mm(a, wk).reshape(T, KV_HEADS, HEAD), pos).astype(jnp.bfloat16)
    v = _mm(a, wv).astype(jnp.bfloat16).reshape(T, KV_HEADS, HEAD)
    o = _attention(q, k, v, seg)
    p = _mm(o, wo).astype(jnp.bfloat16)
    h = (x.astype(jnp.float32) + p.astype(jnp.float32)).astype(jnp.bfloat16)
    b = _rms(h, g2)
    gate = _mm(b, wg).astype(jnp.bfloat16)
    up = _mm(b, wu).astype(jnp.bfloat16)
    u = (jax.nn.silu(gate.astype(jnp.float32)) * up.astype(jnp.float32)).astype(jnp.bfloat16)
    r = _mm(u, wd).astype(jnp.bfloat16)
    y = (h.astype(jnp.float32) + r.astype(jnp.float32)).astype(jnp.bfloat16)
    slots = np.arange(KVR) * KV_HEADS // KVR
    return y, _cache(k[:, slots], l1), _cache(v[:, slots], l1)
```

```python
import functools
import jax
import jax.numpy as jnp
from jax import lax
from jax.experimental import pallas as pl
from jax.experimental.pallas import tpu as pltpu
from jax.sharding import PartitionSpec as P

HEAD = 128
EPS = 1e-5
BASE = 500000.0
CHUNKS = 3
BM = 256
BQ = 256
BK = 512
NEG = -0.7 * float(jnp.finfo(jnp.float32).max)


def _mm(a, b):
    return jnp.dot(a, b, preferred_element_type=jnp.float32)


def _rms(x, g):
    xf = x.astype(jnp.float32)
    ms = jnp.mean(xf * xf, axis=-1, keepdims=True)
    return (xf * lax.rsqrt(ms + EPS) * g.astype(jnp.float32)).astype(jnp.bfloat16)


def _add(x, p):
    return (x.astype(jnp.float32) + p.astype(jnp.float32)).astype(jnp.bfloat16)


def _swiglu(gate, up):
    gate = gate.astype(jnp.bfloat16).astype(jnp.float32)
    up = up.astype(jnp.bfloat16).astype(jnp.float32)
    return (jax.nn.silu(gate) * up).astype(jnp.bfloat16)


def _qkv_body(t_ref, x_ref, g_ref, cos_ref, sin_ref, wq_ref, wk_ref, wv_ref, q_ref, k_ref, v_ref, a_ref):
    xf = x_ref[...].astype(jnp.float32)
    ms = jnp.mean(xf * xf, axis=-1, keepdims=True)
    a_ref[...] = (xf * lax.rsqrt(ms + EPS) * g_ref[...].astype(jnp.float32)).astype(jnp.bfloat16)
    cos = cos_ref[...]
    sin = sin_ref[...]

    def rope(acc, out):
        for h in range(acc.shape[1] // HEAD):
            y = acc[:, h * HEAD:(h + 1) * HEAD]
            out[:, h * HEAD:(h + 1) * HEAD] = (y * cos + pltpu.roll(y, HEAD // 2, 1) * sin).astype(jnp.bfloat16)

    rope(_mm(a_ref[...], wk_ref[...]), k_ref)
    v_ref[...] = _mm(a_ref[...], wv_ref[...]).astype(jnp.bfloat16)
    rope(_mm(a_ref[...], wq_ref[...]), q_ref)


def _qkv(x, g1, cos, sin, wq, wk, wv, t, row0, rows, kvw):
    d = x.shape[1]
    qw = wq.shape[1]
    b0 = row0 // BM
    spec = pltpu.PrefetchScalarGridSpec(
        num_scalar_prefetch=1,
        grid=(rows // BM,),
        in_specs=[
            pl.BlockSpec((BM, d), lambda i, t: (b0 + i, 0)),
            pl.BlockSpec((1, d), lambda i, t: (0, 0)),
            pl.BlockSpec((BM, HEAD), lambda i, t: (b0 + i, 0)),
            pl.BlockSpec((BM, HEAD), lambda i, t: (b0 + i, 0)),
            pl.BlockSpec((d, qw), lambda i, t: (0, 0), pipeline_mode=pl.Buffered(1)),
            pl.BlockSpec((d, kvw), lambda i, t: (0, t[0]), pipeline_mode=pl.Buffered(1)),
            pl.BlockSpec((d, kvw), lambda i, t: (0, t[0]), pipeline_mode=pl.Buffered(1)),
        ],
        out_specs=[
            pl.BlockSpec((BM, qw), lambda i, t: (i, 0)),
            pl.BlockSpec((BM, kvw), lambda i, t: (i, 0)),
            pl.BlockSpec((BM, kvw), lambda i, t: (i, 0)),
        ],
        scratch_shapes=[pltpu.VMEM((BM, d), jnp.bfloat16)],
    )
    return pl.pallas_call(
        _qkv_body,
        grid_spec=spec,
        out_shape=[jax.ShapeDtypeStruct((rows, w), jnp.bfloat16) for w in (qw, kvw, kvw)],
        cost_estimate=pl.CostEstimate(
            flops=2 * rows * d * (qw + 2 * kvw), transcendentals=0,
            bytes_accessed=2 * (rows * d + d * (qw + 2 * kvw))),
        name="qkv",
    )(t, x, g1, cos, sin, wq, wk, wv)


def _attn_body(row0, half, rep, s_ref, q_ref, k_ref, v_ref, o_ref, m_ref, l_ref, acc_ref):
    l1 = s_ref[0]
    core = s_ref[1]
    i = pl.program_id(0)
    nh = half // BQ
    blk = ((i // nh + core) % 2) * nh + i % nh
    q0 = row0 + blk * BQ
    kvl = k_ref.shape[1] // HEAD
    c = HEAD ** -0.5 * 1.4426950408889634
    m_ref[...] = jnp.full_like(m_ref, NEG)
    l_ref[...] = jnp.zeros_like(l_ref)
    acc_ref[...] = jnp.zeros_like(acc_ref)
    first = jnp.where(q0 >= l1, l1, 0) // BK
    last = (q0 + BQ - 1) // BK + 1

    def step(j, masked):
        k0 = pl.multiple_of(j * BK, BK)
        if masked:
            row = q0 + lax.broadcasted_iota(jnp.int32, (BQ, BK), 0)
            col = k0 + lax.broadcasted_iota(jnp.int32, (BQ, BK), 1)
            keep = (col <= row) & (col >= jnp.where(row >= l1, l1, 0))
            keep = jnp.concatenate([keep] * rep, axis=0)
        for g in range(kvl):
            q = jnp.concatenate(
                [q_ref[:, (g * rep + r) * HEAD:(g * rep + r + 1) * HEAD] for r in range(rep)], axis=0)
            kk = k_ref[pl.ds(k0, BK), g * HEAD:(g + 1) * HEAD]
            vv = v_ref[pl.ds(k0, BK), g * HEAD:(g + 1) * HEAD]
            s = lax.dot_general(q, kk, (((1,), (1,)), ((), ())), preferred_element_type=jnp.float32)
            if masked:
                s = jnp.where(keep, s, NEG)
            m_old = m_ref[g]
            m_new = jnp.maximum(m_old, jnp.max(s, axis=-1, keepdims=True))
            m_ref[g] = m_new
            alpha = jnp.exp2((m_old - m_new) * c)
            p = jnp.exp2((s - m_new[:, :1]) * c)
            ps = p[:, :HEAD]
            for z in range(1, BK // HEAD):
                ps = ps + p[:, z * HEAD:(z + 1) * HEAD]
            l_ref[g] = l_ref[g] * alpha + ps
            acc_ref[g] = acc_ref[g] * alpha + _mm(p.astype(jnp.bfloat16), vv)

    def loop(j, carry):
        k0 = j * BK
        one = (q0 >= l1) | (q0 + BQ - 1 < l1)
        clear = (k0 + BK - 1 <= q0) & one & ((q0 < l1) | (k0 >= l1))

        @pl.when(clear)
        def _():
            step(j, False)

        @pl.when(jnp.logical_not(clear))
        def _():
            step(j, True)
        return carry

    lax.fori_loop(first, last, loop, 0)
    for g in range(kvl):
        o = acc_ref[g] / jnp.sum(l_ref[g], axis=-1, keepdims=True)
        for r in range(rep):
            n = g * rep + r
            o_ref[:, n * HEAD:(n + 1) * HEAD] = o[r * BQ:(r + 1) * BQ].astype(jnp.bfloat16)


def _attend(q, k, v, scalars, row0, rep):
    rows, qw = q.shape
    keys, kvw = k.shape
    half = rows // 2
    nh = half // BQ
    kvl = kvw // HEAD
    spec = pltpu.PrefetchScalarGridSpec(
        num_scalar_prefetch=1,
        grid=(rows // BQ,),
        in_specs=[
            pl.BlockSpec((BQ, qw), lambda i, s: (((i // nh + s[1]) % 2) * nh + i % nh, 0)),
            pl.BlockSpec((keys, kvw), lambda i, s: (0, 0)),
            pl.BlockSpec((keys, kvw), lambda i, s: (0, 0)),
        ],
        out_specs=pl.BlockSpec((BQ, qw), lambda i, s: (i, 0)),
        scratch_shapes=[
            pltpu.VMEM((kvl, rep * BQ, HEAD), jnp.float32),
            pltpu.VMEM((kvl, rep * BQ, HEAD), jnp.float32),
            pltpu.VMEM((kvl, rep * BQ, HEAD), jnp.float32),
        ],
    )
    pairs = rows * (row0 + rows // 2) * kvl * rep
    return pl.pallas_call(
        functools.partial(_attn_body, row0, half, rep),
        grid_spec=spec,
        out_shape=jax.ShapeDtypeStruct((rows, qw), jnp.bfloat16),
        cost_estimate=pl.CostEstimate(
            flops=16 * pairs * HEAD, transcendentals=pairs, bytes_accessed=4 * (rows * qw + keys * kvw)),
        name="attend",
    )(scalars, q, k, v)


def _cache(k, l1, kvl):
    n = k.shape[0]
    rows = jnp.arange(n)[:, None]
    z = jnp.zeros((), k.dtype)
    c1 = jnp.where(rows < l1, k, z)
    moved = lax.dynamic_slice_in_dim(jnp.concatenate([k, k]), l1, n, axis=0)
    c2 = jnp.where(rows < n - l1, moved, z)
    return jnp.stack([c1, c2]).reshape(2, n, kvl, HEAD)


def solution(mesh):
    tp = mesh.shape['tp']
    peer = [(i, i ^ 1) for i in range(tp)]
    across = [(i, i ^ 2) for i in range(tp)]

    def layer(x, lens, g1, g2, wq, wk, wv, wo, wg, wu, wd):
        n, d = x.shape
        t = lax.axis_index('tp')
        core = t % 2
        kvl = wk.shape[1] // HEAD // tp
        rep = wq.shape[1] // HEAD // kvl
        l1 = lens[0]
        rows = jnp.arange(n)
        pos = jnp.where(rows >= l1, rows - l1, rows)
        inv = BASE ** (-jnp.arange(0, HEAD, 2, dtype=jnp.float32) / HEAD)
        ang = pos.astype(jnp.float32)[:, None] * jnp.concatenate([inv, inv])[None, :]
        sign = jnp.where(jnp.arange(HEAD) < HEAD // 2, -1.0, 1.0)[None, :]
        cos = jnp.cos(ang)
        sin = jnp.sin(ang) * sign
        scalars = jnp.stack([l1, core]).astype(jnp.int32)
        tv = t.reshape(1).astype(jnp.int32)
        g1r = g1.reshape(1, d)
        cr = n // CHUNKS
        hr = cr // 2

        def reduce(own, other):
            got = lax.ppermute(other, 'tp', peer)
            s = _add(own, got)
            return _add(s, lax.ppermute(s, 'tp', across))

        ks, vs, hs, bs = [], [], [], []
        for c in range(CHUNKS):
            q, k, v = _qkv(x, g1r, cos, sin, wq, wk, wv, tv, c * cr, cr, kvl * HEAD)
            ks.append(k)
            vs.append(v)
            o = _attend(q, jnp.concatenate(ks), jnp.concatenate(vs), scalars, c * cr, rep)
            other = _mm(o[hr:], wo).astype(jnp.bfloat16)
            own = _mm(o[:hr], wo).astype(jnp.bfloat16)
            p = reduce(own, other)
            h = _add(lax.dynamic_slice_in_dim(x, c * cr + core * hr, hr, axis=0), p)
            b = _rms(h, g2)
            hs.append(h)
            bs.append((b, lax.ppermute(b, 'tp', peer)))
        y = jnp.zeros((n, d), jnp.bfloat16)
        for c in range(CHUNKS):
            rs = []
            for b in bs[c]:
                u = _swiglu(_mm(b, wg), _mm(b, wu))
                rs.append(_mm(u, wd).astype(jnp.bfloat16))
            yo = _add(hs[c], reduce(*rs))
            yp = lax.ppermute(yo, 'tp', peer)
            y = lax.dynamic_update_slice_in_dim(y, yo, c * cr + core * hr, axis=0)
            y = lax.dynamic_update_slice_in_dim(y, yp, c * cr + (1 - core) * hr, axis=0)
        return y, _cache(jnp.concatenate(ks), l1, kvl), _cache(jnp.concatenate(vs), l1, kvl)

    row = P('dp', None)
    cache = P('dp', None, 'tp', None)
    return jax.shard_map(
        layer, mesh=mesh,
        in_specs=(row, P('dp'), P(), P(), P(None, 'tp'), P(), P(), P('tp', None),
                  P(None, 'tp'), P(None, 'tp'), P('tp', None)),
        out_specs=(row, cache, cache), check_vma=False)
```

```python
import functools
import jax
import jax.numpy as jnp
from jax import lax
from jax.experimental import pallas as pl
from jax.experimental.pallas import tpu as pltpu
from jax.sharding import PartitionSpec as P

HEAD = 128
EPS = 1e-5
BASE = 500000.0
BM = 256
BQ = 256
BK = 512
NEG = -0.7 * float(jnp.finfo(jnp.float32).max)
F32 = jnp.float32
BF16 = jnp.bfloat16
ANY = pl.BlockSpec(memory_space=pl.ANY)


def _mm(a, b):
    return jnp.dot(a, b, preferred_element_type=F32)


def _cost(flops=0, nbytes=0):
    return pl.CostEstimate(flops=int(flops + 300 * nbytes), transcendentals=0, bytes_accessed=int(nbytes))


def _shape(*s):
    return jax.ShapeDtypeStruct(s, BF16)


def _qkv_body(t_ref, x_ref, g_ref, cos_ref, sin_ref, wq_ref, wk_ref, wv_ref, *refs):
    q_ref, k_ref, v_ref, a_ref = refs[-4:]
    xf = x_ref[...].astype(F32)
    ms = jnp.mean(xf * xf, axis=-1, keepdims=True)
    a_ref[...] = (xf * lax.rsqrt(ms + EPS) * g_ref[...].astype(F32)).astype(BF16)
    cos = cos_ref[...]
    sin = sin_ref[...]

    def rope(acc, out):
        for h in range(acc.shape[1] // HEAD):
            y = acc[:, h * HEAD:(h + 1) * HEAD]
            out[:, h * HEAD:(h + 1) * HEAD] = (y * cos + pltpu.roll(y, HEAD // 2, 1) * sin).astype(BF16)

    rope(_mm(a_ref[...], wk_ref[...]), k_ref)
    v_ref[...] = _mm(a_ref[...], wv_ref[...]).astype(BF16)
    rope(_mm(a_ref[...], wq_ref[...]), q_ref)


def _qkv(x, g1, cos, sin, wq, wk, wv, t, row0, rows, kvw, deps):
    d = x.shape[1]
    qw = wq.shape[1]
    b0 = row0 // BM
    one = pl.Buffered(1)
    spec = pltpu.PrefetchScalarGridSpec(
        num_scalar_prefetch=1,
        grid=(rows // BM,),
        in_specs=[
            pl.BlockSpec((BM, d), lambda i, t: (b0 + i, 0)),
            pl.BlockSpec((1, d), lambda i, t: (0, 0)),
            pl.BlockSpec((BM, HEAD), lambda i, t: (b0 + i, 0)),
            pl.BlockSpec((BM, HEAD), lambda i, t: (b0 + i, 0)),
            pl.BlockSpec((d, qw), lambda i, t: (0, 0), pipeline_mode=one),
            pl.BlockSpec((d, kvw), lambda i, t: (0, t[0]), pipeline_mode=one),
            pl.BlockSpec((d, kvw), lambda i, t: (0, t[0]), pipeline_mode=one),
        ] + [ANY] * len(deps),
        out_specs=[
            pl.BlockSpec((BM, qw), lambda i, t: (i, 0)),
            pl.BlockSpec((BM, kvw), lambda i, t: (i, 0)),
            pl.BlockSpec((BM, kvw), lambda i, t: (i, 0)),
        ],
        scratch_shapes=[pltpu.VMEM((BM, d), BF16)],
    )
    return pl.pallas_call(
        _qkv_body, grid_spec=spec, out_shape=[_shape(rows, w) for w in (qw, kvw, kvw)],
        cost_estimate=_cost(2 * rows * d * (qw + 2 * kvw), 2 * rows * d), name="qkv",
    )(t, x, g1, cos, sin, wq, wk, wv, *deps)


def _join(refs, out):
    at = 0
    for r in refs:
        out[at:at + r.shape[0], :] = r[...]
        at += r.shape[0]


def _attn_body(row0, half, rep, parts, s_ref, q_ref, *refs):
    o_ref, k_ref, v_ref, m_ref, acc_ref = refs[-5:]
    l1 = s_ref[0]
    i = pl.program_id(0)

    @pl.when(i == 0)
    def _():
        _join(refs[:parts], k_ref)
        _join(refs[parts:2 * parts], v_ref)

    nh = half // BQ
    blk = ((i // nh + s_ref[1]) % 2) * nh + i % nh
    q0 = row0 + blk * BQ
    kvl = k_ref.shape[1] // HEAD
    c = HEAD ** -0.5 * 1.4426950408889634
    m_ref[...] = jnp.full_like(m_ref, NEG)
    acc_ref[...] = jnp.zeros_like(acc_ref)
    first = jnp.where(q0 >= l1, l1, 0) // BK
    last = (q0 + BQ - 1) // BK + 1
    ones = jnp.ones((BK, HEAD), BF16)

    def step(j, masked):
        k0 = pl.multiple_of(j * BK, BK)
        if masked:
            row = q0 + lax.broadcasted_iota(jnp.int32, (BQ, BK), 0)
            col = k0 + lax.broadcasted_iota(jnp.int32, (BQ, BK), 1)
            keep = (col <= row) & (col >= jnp.where(row >= l1, l1, 0))
            keep = jnp.concatenate([keep] * rep, axis=0)
        ss = []
        for g in range(kvl):
            q = jnp.concatenate(
                [q_ref[:, (g * rep + r) * HEAD:(g * rep + r + 1) * HEAD] for r in range(rep)], axis=0)
            kk = k_ref[pl.ds(k0, BK), g * HEAD:(g + 1) * HEAD]
            s = lax.dot_general(q, kk, (((1,), (1,)), ((), ())), preferred_element_type=F32)
            ss.append(jnp.where(keep, s, NEG) if masked else s)
        for g in range(kvl):
            s = ss[g]
            m_old = m_ref[g]
            m_new = jnp.maximum(m_old, jnp.max(s, axis=-1, keepdims=True))
            m_ref[g] = m_new
            alpha = jnp.exp2((m_old - m_new) * c)
            p = jnp.exp2((s - m_new[:, :1]) * c).astype(BF16)
            vv = jnp.concatenate([v_ref[pl.ds(k0, BK), g * HEAD:(g + 1) * HEAD], ones], axis=1)
            acc_ref[g] = acc_ref[g] * jnp.concatenate([alpha, alpha], axis=1) + _mm(p, vv)

    def loop(j, carry):
        k0 = j * BK
        one = (q0 >= l1) | (q0 + BQ - 1 < l1)
        clear = (k0 + BK - 1 <= q0) & one & ((q0 < l1) | (k0 >= l1))

        @pl.when(clear)
        def _():
            step(j, False)

        @pl.when(jnp.logical_not(clear))
        def _():
            step(j, True)

        return carry

    lax.fori_loop(first, last, loop, 0)
    for g in range(kvl):
        o = acc_ref[g, :, :HEAD] / acc_ref[g, :, HEAD:]
        for r in range(rep):
            n = g * rep + r
            o_ref[:, n * HEAD:(n + 1) * HEAD] = o[r * BQ:(r + 1) * BQ].astype(BF16)


def _attend(q, k, v, scalars, row0, q_at, rows, rep, deps):
    qw = q.shape[1]
    kvw = k[0].shape[1]
    keys = sum(a.shape[0] for a in k)
    half = rows // 2
    nh = half // BQ
    kvl = kvw // HEAD
    qb = q_at // BQ
    spec = pltpu.PrefetchScalarGridSpec(
        num_scalar_prefetch=1,
        grid=(rows // BQ,),
        in_specs=[
            pl.BlockSpec((BQ, qw), lambda i, s: (qb + ((i // nh + s[1]) % 2) * nh + i % nh, 0)),
        ] + [pl.BlockSpec(a.shape, lambda i, s: (0, 0), pipeline_mode=pl.Buffered(1)) for a in k + v]
        + [ANY] * len(deps),
        out_specs=pl.BlockSpec((BQ, qw), lambda i, s: (i, 0)),
        scratch_shapes=[
            pltpu.VMEM((keys, kvw), BF16),
            pltpu.VMEM((keys, kvw), BF16),
            pltpu.VMEM((kvl, rep * BQ, HEAD), F32),
            pltpu.VMEM((kvl, rep * BQ, 2 * HEAD), F32),
        ],
    )
    pairs = rows * (row0 + rows // 2) * kvl * rep
    return pl.pallas_call(
        functools.partial(_attn_body, row0, half, rep, len(k)), grid_spec=spec, out_shape=_shape(rows, qw),
        cost_estimate=_cost(16 * pairs * HEAD), name="attend",
    )(scalars, q, *k, *v, *deps)


def _proj_body(a_ref, c_ref, w_ref, own_ref, oth_ref):
    oth_ref[...] = _mm(c_ref[...], w_ref[...]).astype(BF16)
    own_ref[...] = _mm(a_ref[...], w_ref[...]).astype(BF16)


def _proj(o, w, bn):
    rows, kd = o.shape
    n = w.shape[1]
    hr = rows // 2
    out = pl.BlockSpec((hr, bn), lambda j: (0, j))
    return pl.pallas_call(
        _proj_body, grid=(n // bn,),
        in_specs=[
            pl.BlockSpec((hr, kd), lambda j: (0, 0), pipeline_mode=pl.Buffered(1)),
            pl.BlockSpec((hr, kd), lambda j: (1, 0), pipeline_mode=pl.Buffered(1)),
            pl.BlockSpec((kd, bn), lambda j: (0, j)),
        ],
        out_specs=[out, out], out_shape=[_shape(hr, n)] * 2,
        cost_estimate=_cost(2 * rows * kd * n), name="proj",
    )(o, o, w)


def _mlp_body(ng, bf, bo_ref, bp_ref, wg_ref, wu_ref, wd_ref, *refs):
    own_ref, oth_ref, u_ref = refs[-3:]
    i = pl.program_id(0)
    hr = bo_ref.shape[0]

    @pl.when(i < ng)
    def _():
        for z, b_ref in enumerate((bo_ref, bp_ref)):
            gate = _mm(b_ref[...], wg_ref[...]).astype(BF16).astype(F32)
            up = _mm(b_ref[...], wu_ref[...]).astype(BF16).astype(F32)
            u_ref[z * hr:(z + 1) * hr, pl.ds(pl.multiple_of(i * bf, bf), bf)] = (jax.nn.silu(gate) * up).astype(BF16)

    @pl.when(i >= ng)
    def _():
        for z, out in ((1, oth_ref), (0, own_ref)):
            out[...] = _mm(u_ref[z * hr:(z + 1) * hr, :], wd_ref[...]).astype(BF16)


def _mlp(bo, bp, wg, wu, wd, deps):
    hr, d = bo.shape
    f = wg.shape[1]
    bf, bn = 256, 512
    ng, nd = f // bf, d // bn
    out = pl.BlockSpec((hr, bn), lambda i: (0, jnp.maximum(i - ng, 0)))
    rows = pl.BlockSpec((hr, d), lambda i: (0, 0), pipeline_mode=pl.Buffered(1))
    cols = pl.BlockSpec((d, bf), lambda i: (0, jnp.minimum(i, ng - 1)))
    return pl.pallas_call(
        functools.partial(_mlp_body, ng, bf), grid=(ng + nd,),
        in_specs=[rows, rows, cols, cols, pl.BlockSpec((f, bn), lambda i: (0, jnp.maximum(i - ng, 0)))]
        + [ANY] * len(deps),
        out_specs=[out, out], out_shape=[_shape(hr, d)] * 2,
        scratch_shapes=[pltpu.VMEM((2 * hr, f), BF16)],
        compiler_params=pltpu.CompilerParams(vmem_limit_bytes=60 * 1024 * 1024),
        cost_estimate=_cost(12 * hr * d * f), name="mlp",
    )(bo, bp, wg, wu, wd, *deps)


def _sum(a, b):
    return (a.astype(F32) + b.astype(F32)).astype(BF16)


def _add_body(a_ref, b_ref, o_ref):
    o_ref[...] = _sum(a_ref[...], b_ref[...])


def _add(a, b):
    hr, d = a.shape
    blk = pl.BlockSpec((hr // 4, d), lambda i: (i, 0))
    return pl.pallas_call(
        _add_body, grid=(4,), in_specs=[blk, blk], out_specs=blk, out_shape=_shape(hr, d),
        cost_estimate=_cost(0, 6 * hr * d), name="add",
    )(a, b)


def _hb_body(s_ref, x_ref, p_ref, q_ref, g_ref, h_ref, b_ref):
    h = _sum(x_ref[...], _sum(p_ref[...], q_ref[...]))
    h_ref[...] = h
    hf = h.astype(F32)
    ms = jnp.mean(hf * hf, axis=-1, keepdims=True)
    b_ref[...] = (hf * lax.rsqrt(ms + EPS) * g_ref[...].astype(F32)).astype(BF16)


def _hb(x, p, q, g2, scalars, row0):
    hr, d = p.shape
    rb = hr // 4
    blk = pl.BlockSpec((rb, d), lambda i, s: (i, 0))
    return pl.pallas_call(
        _hb_body,
        grid_spec=pltpu.PrefetchScalarGridSpec(
            num_scalar_prefetch=1, grid=(4,),
            in_specs=[pl.BlockSpec((rb, d), lambda i, s: (row0 // rb + s[1] * 4 + i, 0)), blk, blk,
                      pl.BlockSpec((1, d), lambda i, s: (0, 0))],
            out_specs=[blk, blk]),
        out_shape=[_shape(hr, d)] * 2, cost_estimate=_cost(0, 10 * hr * d), name="hb",
    )(scalars, x, p, q, g2)


def _y_body(s_ref, h_ref, p_ref, q_ref, *refs):
    o_ref, y_ref = refs[-2:]
    y = _sum(h_ref[...], _sum(p_ref[...], q_ref[...]))
    o_ref[...] = y
    y_ref[...] = y


def _y(h, p, q, y, n, scalars, row0):
    hr, d = p.shape
    rb = hr // 4
    blk = pl.BlockSpec((rb, d), lambda i, s: (i, 0))
    old = [] if y is None else [y]
    return pl.pallas_call(
        _y_body,
        grid_spec=pltpu.PrefetchScalarGridSpec(
            num_scalar_prefetch=1, grid=(4,), in_specs=[blk, blk, blk] + [ANY] * len(old),
            out_specs=[blk, pl.BlockSpec((rb, d), lambda i, s: (row0 // rb + s[1] * 4 + i, 0))]),
        out_shape=[_shape(hr, d), _shape(n, d)],
        input_output_aliases={} if y is None else {4: 1},
        cost_estimate=_cost(0, 10 * hr * d), name="resid",
    )(scalars, h, p, q, *old)


def _put_body(s_ref, a_ref, y_in, y_ref):
    y_ref[...] = a_ref[...]


def _put(a, y, scalars, row0):
    hr, d = a.shape
    rb = hr // 4
    return pl.pallas_call(
        _put_body,
        grid_spec=pltpu.PrefetchScalarGridSpec(
            num_scalar_prefetch=1, grid=(4,), in_specs=[pl.BlockSpec((rb, d), lambda i, s: (i, 0)), ANY],
            out_specs=pl.BlockSpec((rb, d), lambda i, s: (row0 // rb + (1 - s[1]) * 4 + i, 0))),
        out_shape=_shape(*y.shape), input_output_aliases={2: 0},
        cost_estimate=_cost(0, 4 * hr * d), name="put",
    )(scalars, a, y)


def _cache_body(rb, parts, s_ref, *refs):
    ko_ref, vo_ref, k_ref, v_ref = refs[-4:]
    l1 = s_ref[0]
    n = k_ref.shape[0]
    seg = pl.program_id(0)
    r0 = pl.program_id(1) * rb

    @pl.when((seg == 0) & (r0 == 0))
    def _():
        _join(refs[:parts], k_ref)
        _join(refs[parts:2 * parts], v_ref)

    size = jnp.where(seg == 0, l1, n - l1)
    off = r0 + seg * l1
    at = pl.multiple_of(jnp.minimum(off // 16 * 16, n - rb - 16), 16)
    turn = (2 * (rb + 16) - jnp.minimum(off - at, rb + 16)) % (rb + 16)
    keep = r0 + lax.broadcasted_iota(jnp.int32, (rb, k_ref.shape[1]), 0) < size
    for src, out in ((k_ref, ko_ref), (v_ref, vo_ref)):
        a = pltpu.roll(src[pl.ds(at, rb + 16), :].astype(F32), turn, 0)[:rb]
        out[...] = jnp.where(keep, a, 0.0).astype(BF16)


def _cache(k, v, scalars, n, kvw, deps):
    rb = 512
    out = pl.BlockSpec((rb, kvw), lambda g, i, s: (g * (n // rb) + i, 0))
    return pl.pallas_call(
        functools.partial(_cache_body, rb, len(k)),
        grid_spec=pltpu.PrefetchScalarGridSpec(
            num_scalar_prefetch=1, grid=(2, n // rb),
            in_specs=[pl.BlockSpec(a.shape, lambda g, i, s: (0, 0), pipeline_mode=pl.Buffered(1)) for a in k + v]
            + [ANY] * len(deps),
            out_specs=[out, out],
            scratch_shapes=[pltpu.VMEM((n, kvw), BF16), pltpu.VMEM((n, kvw), BF16)]),
        out_shape=[_shape(2 * n, kvw)] * 2, cost_estimate=_cost(0, 12 * n * kvw), name="cache",
    )(scalars, *k, *v, *deps)


def solution(mesh):
    tp = mesh.shape['tp']
    peer = [(i, i ^ 1) for i in range(tp)]
    across = [(i, i ^ 2) for i in range(tp)]

    def layer(x, lens, g1, g2, wq, wk, wv, wo, wg, wu, wd):
        n, d = x.shape
        t = lax.axis_index('tp')
        core = t % 2
        kvl = wk.shape[1] // HEAD // tp
        kvw = kvl * HEAD
        rep = wq.shape[1] // HEAD // kvl
        l1 = lens[0]
        rows = jnp.arange(n)
        pos = jnp.where(rows >= l1, rows - l1, rows)
        inv = BASE ** (-jnp.arange(0, HEAD, 2, dtype=F32) / HEAD)
        ang = pos.astype(F32)[:, None] * jnp.concatenate([inv, inv])[None, :]
        sign = jnp.where(jnp.arange(HEAD) < HEAD // 2, -1.0, 1.0)[None, :]
        cos = jnp.cos(ang)
        sin = jnp.sin(ang) * sign
        sc = jnp.stack([l1, core]).astype(jnp.int32)
        tv = t.reshape(1).astype(jnp.int32)
        g1r = g1.reshape(1, d)
        g2r = g2.reshape(1, d)
        e = n // 6
        start = [0, e, 3 * e, 5 * e]
        size = [e, 2 * e, 2 * e, e]

        def move(a, perm):
            return lax.ppermute(a, 'tp', perm)

        def qkv(row0, m, *deps):
            return _qkv(x, g1r, cos, sin, wq, wk, wv, tv, row0, m, kvw, deps)

        def att(c, q, q_at, k, v, *deps):
            o = _attend(q, k, v, sc, start[c], q_at, size[c], rep, deps)
            return _proj(o, wo, 1280)

        def mlp(b, *deps):
            other = move(b, peer)
            return _mlp(b, other, wg, wu, wd, deps)

        def half(pair):
            own, other = pair
            other = move(other, peer)
            s = _add(own, other)
            return s, move(s, across)

        def hb(c, s):
            return _hb(x, *s, g2r, sc, start[c])

        def resid(c, h, s, y):
            own, y = _y(h, *s, y, n, sc, start[c])
            return y, move(own, peer)

        def put(c, y, other):
            return _put(other, y, sc, start[c])

        q0, k0, v0 = qkv(0, e)
        p0 = att(0, q0, 0, [k0], [v0])
        q1, k1, v1 = qkv(e, 2 * e, p0[1])
        s0 = half(p0)
        p1 = att(1, q1, 0, [k0, k1], [v0, v1], s0[0])
        q2, k2, v2 = qkv(3 * e, 3 * e, p1[1])
        k, v = [k0, k1, k2], [v0, v1, v2]
        s1 = half(p1)
        p2 = att(2, q2, 0, k, v, s1[0])
        h0, b0 = hb(0, s0)
        s2 = half(p2)
        p3 = att(3, q2, 2 * e, k, v, s2[0], b0)
        h1, b1 = hb(1, s1)
        r0 = mlp(b0, p3[1], b1)
        s3 = half(p3)
        t0 = half(r0)
        r1 = mlp(b1, s3[0], t0[0])
        h2, b2 = hb(2, s2)
        t1 = half(r1)
        h3, b3 = hb(3, s3)
        r2 = mlp(b2, t1[0], b3)
        t2 = half(r2)
        y, other = resid(0, h0, t0, None)
        r3 = mlp(b3, t2[0], y)
        y = put(0, y, other)
        t3 = half(r3)
        for c, h, t in ((1, h1, t1), (2, h2, t2), (3, h3, t3)):
            y = put(c, *resid(c, h, t, y))
        kc, vc = _cache(k, v, sc, n, kvw, (t3[0],))
        shape = (2, n, kvl, HEAD)
        return y, kc.reshape(shape), vc.reshape(shape)

    row = P('dp', None)
    cache = P('dp', None, 'tp', None)
    return jax.shard_map(
        layer, mesh=mesh,
        in_specs=(row, P('dp'), P(), P(), P(None, 'tp'), P(), P(), P('tp', None),
                  P(None, 'tp'), P(None, 'tp'), P('tp', None)),
        out_specs=(row, cache, cache), check_vma=False)
```

```python
import functools
import jax
import jax.numpy as jnp
from jax import lax
from jax.experimental import pallas as pl
from jax.experimental.pallas import tpu as pltpu
from jax.sharding import PartitionSpec as P

HEAD = 128
EPS = 1e-5
BASE = 500000.0
BM = 256
BQ = 256
BK = 512
NEG = -0.7 * float(jnp.finfo(jnp.float32).max)
F32 = jnp.float32
BF16 = jnp.bfloat16
ANY = pl.BlockSpec(memory_space=pl.ANY)


def _mm(a, b):
    return jnp.dot(a, b, preferred_element_type=F32)


def _cost(flops=0, nbytes=0):
    return pl.CostEstimate(flops=int(flops + 300 * nbytes), transcendentals=0, bytes_accessed=int(nbytes))


def _shape(*s):
    return jax.ShapeDtypeStruct(s, BF16)


def _qkv_body(t_ref, x_ref, g_ref, cos_ref, sin_ref, wq_ref, wk_ref, wv_ref, *refs):
    q_ref, k_ref, v_ref, a_ref = refs[-4:]
    xf = x_ref[...].astype(F32)
    ms = jnp.mean(xf * xf, axis=-1, keepdims=True)
    a_ref[...] = (xf * lax.rsqrt(ms + EPS) * g_ref[...].astype(F32)).astype(BF16)
    cos = cos_ref[...]
    sin = sin_ref[...]

    def rope(acc, out):
        for h in range(acc.shape[1] // HEAD):
            y = acc[:, h * HEAD:(h + 1) * HEAD]
            out[:, h * HEAD:(h + 1) * HEAD] = (y * cos + pltpu.roll(y, HEAD // 2, 1) * sin).astype(BF16)

    rope(_mm(a_ref[...], wk_ref[...]), k_ref)
    v_ref[...] = _mm(a_ref[...], wv_ref[...]).astype(BF16)
    rope(_mm(a_ref[...], wq_ref[...]), q_ref)


def _qkv(x, g1, cos, sin, wq, wk, wv, t, row0, rows, kvw, deps):
    d = x.shape[1]
    qw = wq.shape[1]
    b0 = row0 // BM
    one = pl.Buffered(1)
    spec = pltpu.PrefetchScalarGridSpec(
        num_scalar_prefetch=1,
        grid=(rows // BM,),
        in_specs=[
            pl.BlockSpec((BM, d), lambda i, t: (b0 + i, 0)),
            pl.BlockSpec((1, d), lambda i, t: (0, 0)),
            pl.BlockSpec((BM, HEAD), lambda i, t: (b0 + i, 0)),
            pl.BlockSpec((BM, HEAD), lambda i, t: (b0 + i, 0)),
            pl.BlockSpec((d, qw), lambda i, t: (0, 0), pipeline_mode=one),
            pl.BlockSpec((d, kvw), lambda i, t: (0, t[0]), pipeline_mode=one),
            pl.BlockSpec((d, kvw), lambda i, t: (0, t[0]), pipeline_mode=one),
        ] + [ANY] * len(deps),
        out_specs=[
            pl.BlockSpec((BM, qw), lambda i, t: (i, 0)),
            pl.BlockSpec((BM, kvw), lambda i, t: (i, 0)),
            pl.BlockSpec((BM, kvw), lambda i, t: (i, 0)),
        ],
        scratch_shapes=[pltpu.VMEM((BM, d), BF16)],
    )
    return pl.pallas_call(
        _qkv_body, grid_spec=spec, out_shape=[_shape(rows, w) for w in (qw, kvw, kvw)],
        cost_estimate=_cost(2 * rows * d * (qw + 2 * kvw), 2 * rows * d), name="qkv",
    )(t, x, g1, cos, sin, wq, wk, wv, *deps)


def _join(refs, out):
    at = 0
    for r in refs:
        out[at:at + r.shape[0], :] = r[...]
        at += r.shape[0]


def _attn_body(row0, half, rep, parts, s_ref, q_ref, *refs):
    own_ref, oth_ref, k_ref, v_ref, m_ref, acc_ref = refs[-6:]
    l1 = s_ref[0]
    i = pl.program_id(0)

    @pl.when(i == 0)
    def _():
        _join(refs[:parts], k_ref)
        _join(refs[parts:2 * parts], v_ref)

    nh = half // BQ
    blk = ((i // nh + s_ref[1]) % 2) * nh + i % nh
    q0 = row0 + blk * BQ
    kvl = k_ref.shape[1] // HEAD
    c = HEAD ** -0.5 * 1.4426950408889634
    m_ref[...] = jnp.full_like(m_ref, NEG)
    acc_ref[...] = jnp.zeros_like(acc_ref)
    first = jnp.where(q0 >= l1, l1, 0) // BK
    last = (q0 + BQ - 1) // BK + 1
    ones = jnp.ones((BK, HEAD), BF16)

    def step(j, masked):
        k0 = pl.multiple_of(j * BK, BK)
        if masked:
            row = q0 + lax.broadcasted_iota(jnp.int32, (BQ, BK), 0)
            col = k0 + lax.broadcasted_iota(jnp.int32, (BQ, BK), 1)
            keep = (col <= row) & (col >= jnp.where(row >= l1, l1, 0))
            keep = jnp.concatenate([keep] * rep, axis=0)
        ss = []
        for g in range(kvl):
            q = jnp.concatenate(
                [q_ref[:, (g * rep + r) * HEAD:(g * rep + r + 1) * HEAD] for r in range(rep)], axis=0)
            kk = k_ref[pl.ds(k0, BK), g * HEAD:(g + 1) * HEAD]
            s = lax.dot_general(q, kk, (((1,), (1,)), ((), ())), preferred_element_type=F32)
            ss.append(jnp.where(keep, s, NEG) if masked else s)
        for g in range(kvl):
            s = ss[g]
            m_old = m_ref[g]
            m_new = jnp.maximum(m_old, jnp.max(s, axis=-1, keepdims=True))
            m_ref[g] = m_new
            alpha = jnp.exp2((m_old - m_new) * c)
            p = jnp.exp2((s - m_new[:, :1]) * c).astype(BF16)
            vv = jnp.concatenate([v_ref[pl.ds(k0, BK), g * HEAD:(g + 1) * HEAD], ones], axis=1)
            acc_ref[g] = acc_ref[g] * jnp.concatenate([alpha, alpha], axis=1) + _mm(p, vv)

    def loop(j, carry):
        k0 = j * BK
        one = (q0 >= l1) | (q0 + BQ - 1 < l1)
        clear = (k0 + BK - 1 <= q0) & one & ((q0 < l1) | (k0 >= l1))

        @pl.when(clear)
        def _():
            step(j, False)

        @pl.when(jnp.logical_not(clear))
        def _():
            step(j, True)

        return carry

    lax.fori_loop(first, last, loop, 0)

    def store(o_ref):
        for g in range(kvl):
            o = acc_ref[g, :, :HEAD] / acc_ref[g, :, HEAD:]
            for r in range(rep):
                n = g * rep + r
                o_ref[:, n * HEAD:(n + 1) * HEAD] = o[r * BQ:(r + 1) * BQ].astype(BF16)

    @pl.when(i < nh)
    def _():
        store(own_ref)

    @pl.when(i >= nh)
    def _():
        store(oth_ref)


def _attend(q, k, v, scalars, row0, q_at, rows, rep, deps):
    qw = q.shape[1]
    kvw = k[0].shape[1]
    keys = sum(a.shape[0] for a in k)
    half = rows // 2
    nh = half // BQ
    kvl = kvw // HEAD
    qb = q_at // BQ
    spec = pltpu.PrefetchScalarGridSpec(
        num_scalar_prefetch=1,
        grid=(rows // BQ,),
        in_specs=[
            pl.BlockSpec((BQ, qw), lambda i, s: (qb + ((i // nh + s[1]) % 2) * nh + i % nh, 0)),
        ] + [pl.BlockSpec(a.shape, lambda i, s: (0, 0), pipeline_mode=pl.Buffered(1)) for a in k + v]
        + [ANY] * len(deps),
        out_specs=[
            pl.BlockSpec((BQ, qw), lambda i, s: (jnp.minimum(i, nh - 1), 0)),
            pl.BlockSpec((BQ, qw), lambda i, s: (jnp.maximum(i - nh, 0), 0)),
        ],
        scratch_shapes=[
            pltpu.VMEM((keys, kvw), BF16),
            pltpu.VMEM((keys, kvw), BF16),
            pltpu.VMEM((kvl, rep * BQ, HEAD), F32),
            pltpu.VMEM((kvl, rep * BQ, 2 * HEAD), F32),
        ],
    )
    pairs = rows * (row0 + rows // 2) * kvl * rep
    return pl.pallas_call(
        functools.partial(_attn_body, row0, half, rep, len(k)), grid_spec=spec, out_shape=[_shape(half, qw)] * 2,
        cost_estimate=_cost(16 * pairs * HEAD), name="attend",
    )(scalars, q, *k, *v, *deps)


def _proj_body(a_ref, c_ref, w_ref, z_ref, o_ref):
    o_ref[...] = (_mm(a_ref[...], w_ref[...]) + _mm(c_ref[...], z_ref[...])).astype(BF16)


def _proj(a, c, w, z, bn):
    hr, kd = a.shape
    n = w.shape[1]
    rows = pl.BlockSpec((hr, kd), lambda j: (0, 0), pipeline_mode=pl.Buffered(1))
    cols = pl.BlockSpec((kd, bn), lambda j: (0, j))
    return pl.pallas_call(
        _proj_body, grid=(n // bn,), in_specs=[rows, rows, cols, cols],
        out_specs=pl.BlockSpec((hr, bn), lambda j: (0, j)), out_shape=_shape(hr, n),
        cost_estimate=_cost(4 * hr * kd * n), name="proj",
    )(a, c, w, z)


def _mlp_body(ng, bf, b_ref, wg_ref, wu_ref, zg_ref, zu_ref, wd_ref, zd_ref, *refs):
    o_ref, u_ref = refs[-2:]
    i = pl.program_id(0)
    f = ng * bf

    def gate_up(g_ref, up_ref):
        gate = _mm(b_ref[...], g_ref[...]).astype(BF16).astype(F32)
        up = _mm(b_ref[...], up_ref[...]).astype(BF16).astype(F32)
        u_ref[:, pl.ds(pl.multiple_of(i * bf, bf), bf)] = (jax.nn.silu(gate) * up).astype(BF16)

    @pl.when(i < ng)
    def _():
        gate_up(wg_ref, wu_ref)

    @pl.when((i >= ng) & (i < 2 * ng))
    def _():
        gate_up(zg_ref, zu_ref)

    @pl.when(i >= 2 * ng)
    def _():
        o_ref[...] = (_mm(u_ref[:, :f], wd_ref[...]) + _mm(u_ref[:, f:], zd_ref[...])).astype(BF16)


def _mlp(b, w, z, deps):
    hr, d = b.shape
    f = w[0].shape[1]
    bf, bn = 256, 512
    ng, nd = f // bf, d // bn
    down = lambda i: (0, jnp.maximum(i - 2 * ng, 0))
    mine = pl.BlockSpec((d, bf), lambda i: (0, jnp.minimum(i, ng - 1)))
    other = pl.BlockSpec((d, bf), lambda i: (0, jnp.clip(i - ng, 0, ng - 1)))
    cols = pl.BlockSpec((f, bn), down)
    return pl.pallas_call(
        functools.partial(_mlp_body, ng, bf), grid=(2 * ng + nd,),
        in_specs=[pl.BlockSpec((hr, d), lambda i: (0, 0), pipeline_mode=pl.Buffered(1)),
                  mine, mine, other, other, cols, cols] + [ANY] * len(deps),
        out_specs=pl.BlockSpec((hr, bn), down), out_shape=_shape(hr, d),
        scratch_shapes=[pltpu.VMEM((hr, 2 * f), BF16)],
        compiler_params=pltpu.CompilerParams(vmem_limit_bytes=60 * 1024 * 1024),
        cost_estimate=_cost(12 * hr * d * f), name="mlp",
    )(b, w[0], w[1], z[0], z[1], w[2], z[2], *deps)


def _sum(a, b):
    return (a.astype(F32) + b.astype(F32)).astype(BF16)


def _hb_body(s_ref, x_ref, p_ref, q_ref, g_ref, h_ref, b_ref):
    h = _sum(x_ref[...], _sum(p_ref[...], q_ref[...]))
    h_ref[...] = h
    hf = h.astype(F32)
    ms = jnp.mean(hf * hf, axis=-1, keepdims=True)
    b_ref[...] = (hf * lax.rsqrt(ms + EPS) * g_ref[...].astype(F32)).astype(BF16)


def _hb(x, p, q, g2, scalars, row0):
    hr, d = p.shape
    rb = hr // 4
    blk = pl.BlockSpec((rb, d), lambda i, s: (i, 0))
    return pl.pallas_call(
        _hb_body,
        grid_spec=pltpu.PrefetchScalarGridSpec(
            num_scalar_prefetch=1, grid=(4,),
            in_specs=[pl.BlockSpec((rb, d), lambda i, s: (row0 // rb + s[1] * 4 + i, 0)), blk, blk,
                      pl.BlockSpec((1, d), lambda i, s: (0, 0))],
            out_specs=[blk, blk]),
        out_shape=[_shape(hr, d)] * 2, cost_estimate=_cost(0, 10 * hr * d), name="hb",
    )(scalars, x, p, q, g2)


def _y_body(s_ref, h_ref, p_ref, q_ref, *refs):
    o_ref, y_ref = refs[-2:]
    y = _sum(h_ref[...], _sum(p_ref[...], q_ref[...]))
    o_ref[...] = y
    y_ref[...] = y


def _y(h, p, q, y, n, scalars, row0):
    hr, d = p.shape
    rb = hr // 4
    blk = pl.BlockSpec((rb, d), lambda i, s: (i, 0))
    old = [] if y is None else [y]
    return pl.pallas_call(
        _y_body,
        grid_spec=pltpu.PrefetchScalarGridSpec(
            num_scalar_prefetch=1, grid=(4,), in_specs=[blk, blk, blk] + [ANY] * len(old),
            out_specs=[blk, pl.BlockSpec((rb, d), lambda i, s: (row0 // rb + s[1] * 4 + i, 0))]),
        out_shape=[_shape(hr, d), _shape(n, d)],
        input_output_aliases={} if y is None else {4: 1},
        cost_estimate=_cost(0, 10 * hr * d), name="resid",
    )(scalars, h, p, q, *old)


def _put_body(s_ref, a_ref, y_in, y_ref):
    y_ref[...] = a_ref[...]


def _put(a, y, scalars, row0):
    hr, d = a.shape
    rb = hr // 4
    return pl.pallas_call(
        _put_body,
        grid_spec=pltpu.PrefetchScalarGridSpec(
            num_scalar_prefetch=1, grid=(4,), in_specs=[pl.BlockSpec((rb, d), lambda i, s: (i, 0)), ANY],
            out_specs=pl.BlockSpec((rb, d), lambda i, s: (row0 // rb + (1 - s[1]) * 4 + i, 0))),
        out_shape=_shape(*y.shape), input_output_aliases={2: 0},
        cost_estimate=_cost(0, 4 * hr * d), name="put",
    )(scalars, a, y)


def _cache_body(rb, parts, s_ref, *refs):
    ko_ref, vo_ref, k_ref, v_ref = refs[-4:]
    l1 = s_ref[0]
    n = k_ref.shape[0]
    seg = pl.program_id(0)
    r0 = pl.program_id(1) * rb

    @pl.when((seg == 0) & (r0 == 0))
    def _():
        _join(refs[:parts], k_ref)
        _join(refs[parts:2 * parts], v_ref)

    size = jnp.where(seg == 0, l1, n - l1)
    off = r0 + seg * l1
    at = pl.multiple_of(jnp.minimum(off // 16 * 16, n - rb - 16), 16)
    turn = (2 * (rb + 16) - jnp.minimum(off - at, rb + 16)) % (rb + 16)
    keep = r0 + lax.broadcasted_iota(jnp.int32, (rb, k_ref.shape[1]), 0) < size
    for src, out in ((k_ref, ko_ref), (v_ref, vo_ref)):
        a = pltpu.roll(src[pl.ds(at, rb + 16), :].astype(F32), turn, 0)[:rb]
        out[...] = jnp.where(keep, a, 0.0).astype(BF16)


def _cache(k, v, scalars, n, kvw, deps):
    rb = 512
    out = pl.BlockSpec((rb, kvw), lambda g, i, s: (g * (n // rb) + i, 0))
    return pl.pallas_call(
        functools.partial(_cache_body, rb, len(k)),
        grid_spec=pltpu.PrefetchScalarGridSpec(
            num_scalar_prefetch=1, grid=(2, n // rb),
            in_specs=[pl.BlockSpec(a.shape, lambda g, i, s: (0, 0), pipeline_mode=pl.Buffered(1)) for a in k + v]
            + [ANY] * len(deps),
            out_specs=[out, out],
            scratch_shapes=[pltpu.VMEM((n, kvw), BF16), pltpu.VMEM((n, kvw), BF16)]),
        out_shape=[_shape(2 * n, kvw)] * 2, cost_estimate=_cost(0, 12 * n * kvw), name="cache",
    )(scalars, *k, *v, *deps)


def solution(mesh):
    tp = mesh.shape['tp']
    peer = [(i, i ^ 1) for i in range(tp)]
    across = [(i, i ^ 2) for i in range(tp)]

    def layer(x, lens, g1, g2, wq, wk, wv, wo, wg, wu, wd):
        n, d = x.shape
        t = lax.axis_index('tp')
        core = t % 2
        kvl = wk.shape[1] // HEAD // tp
        kvw = kvl * HEAD
        rep = wq.shape[1] // HEAD // kvl
        l1 = lens[0]
        rows = jnp.arange(n)
        pos = jnp.where(rows >= l1, rows - l1, rows)
        inv = BASE ** (-jnp.arange(0, HEAD, 2, dtype=F32) / HEAD)
        ang = pos.astype(F32)[:, None] * jnp.concatenate([inv, inv])[None, :]
        sign = jnp.where(jnp.arange(HEAD) < HEAD // 2, -1.0, 1.0)[None, :]
        cos = jnp.cos(ang)
        sin = jnp.sin(ang) * sign
        sc = jnp.stack([l1, core]).astype(jnp.int32)
        tv = t.reshape(1).astype(jnp.int32)
        g1r = g1.reshape(1, d)
        g2r = g2.reshape(1, d)
        e = n // 6
        start = [0, e, 3 * e, 5 * e]
        size = [e, 2 * e, 2 * e, e]

        def move(a, perm):
            return lax.ppermute(a, 'tp', perm)

        def qkv(row0, m, *deps):
            return _qkv(x, g1r, cos, sin, wq, wk, wv, tv, row0, m, kvw, deps)

        def att(c, q, q_at, k, v, *deps):
            own, other = _attend(q, k, v, sc, start[c], q_at, size[c], rep, deps)
            other = move(other, peer)
            return own, other

        def proj(o):
            p = _proj(*o, wo, zo, 640)
            return p, move(p, across)

        def mlp(b, *deps):
            r = _mlp(b, (wg, wu, wd), (zg, zu, zd), deps)
            return r, move(r, across)

        def hb(c, s):
            return _hb(x, *s, g2r, sc, start[c])

        def resid(c, h, s, y):
            own, y = _y(h, *s, y, n, sc, start[c])
            return y, move(own, peer)

        def put(c, y, other):
            return _put(other, y, sc, start[c])

        zo = move(wo, peer)
        zg = move(wg, peer)
        zu = move(wu, peer)
        zd = move(wd, peer)
        q0, k0, v0 = qkv(0, e)
        p0 = proj(att(0, q0, 0, [k0], [v0]))
        q1, k1, v1 = qkv(e, 2 * e, p0[0])
        p1 = proj(att(1, q1, 0, [k0, k1], [v0, v1]))
        q2, k2, v2 = qkv(3 * e, 3 * e, p1[0])
        k, v = [k0, k1, k2], [v0, v1, v2]
        o2 = att(2, q2, 0, k, v)
        h0, b0 = hb(0, p0)
        p2 = proj(o2)
        p3 = proj(att(3, q2, 2 * e, k, v, p2[0], b0))
        r0 = mlp(b0, p3[0])
        h1, b1 = hb(1, p1)
        r1 = mlp(b1, r0[0])
        h2, b2 = hb(2, p2)
        r2 = mlp(b2, r1[0])
        h3, b3 = hb(3, p3)
        y, other = resid(0, h0, r0, None)
        r3 = mlp(b3, r2[0], y)
        y = put(0, y, other)
        for c, h, r in ((1, h1, r1), (2, h2, r2), (3, h3, r3)):
            y = put(c, *resid(c, h, r, y))
        kc, vc = _cache(k, v, sc, n, kvw, (r3[0],))
        shape = (2, n, kvl, HEAD)
        return y, kc.reshape(shape), vc.reshape(shape)

    row = P('dp', None)
    cache = P('dp', None, 'tp', None)
    return jax.shard_map(
        layer, mesh=mesh,
        in_specs=(row, P('dp'), P(), P(), P(None, 'tp'), P(), P(), P('tp', None),
                  P(None, 'tp'), P(None, 'tp'), P('tp', None)),
        out_specs=(row, cache, cache), check_vma=False)
```

```python
import functools
import jax
import jax.numpy as jnp
from jax import lax
from jax.experimental import pallas as pl
from jax.experimental.pallas import tpu as pltpu
from jax.sharding import PartitionSpec as P

HEAD = 128
EPS = 1e-5
BASE = 500000.0
BM = 256
BQ = 384
BK = 512
NEG = -0.7 * float(jnp.finfo(jnp.float32).max)
F32 = jnp.float32
BF16 = jnp.bfloat16
ANY = pl.BlockSpec(memory_space=pl.ANY)


def _mm(a, b):
    return jnp.dot(a, b, preferred_element_type=F32)


def _cost(flops=0, nbytes=0):
    return pl.CostEstimate(flops=int(flops + 300 * nbytes), transcendentals=0, bytes_accessed=int(nbytes))


def _shape(*s):
    return jax.ShapeDtypeStruct(s, BF16)


def _qkv_body(t_ref, x_ref, g_ref, cos_ref, sin_ref, wq_ref, wk_ref, wv_ref, *refs):
    q_ref, k_ref, v_ref, a_ref = refs[-4:]
    xf = x_ref[...].astype(F32)
    ms = jnp.mean(xf * xf, axis=-1, keepdims=True)
    a_ref[...] = (xf * lax.rsqrt(ms + EPS) * g_ref[...].astype(F32)).astype(BF16)
    cos = cos_ref[...]
    sin = sin_ref[...]

    def rope(acc, out):
        for h in range(acc.shape[1] // HEAD):
            y = acc[:, h * HEAD:(h + 1) * HEAD]
            out[:, h * HEAD:(h + 1) * HEAD] = (y * cos + pltpu.roll(y, HEAD // 2, 1) * sin).astype(BF16)

    rope(_mm(a_ref[...], wk_ref[...]), k_ref)
    v_ref[...] = _mm(a_ref[...], wv_ref[...]).astype(BF16)
    rope(_mm(a_ref[...], wq_ref[...]), q_ref)


def _qkv(x, g1, cos, sin, wq, wk, wv, t, row0, rows, kvw, deps):
    d = x.shape[1]
    qw = wq.shape[1]
    b0 = row0 // BM
    one = pl.Buffered(1)
    spec = pltpu.PrefetchScalarGridSpec(
        num_scalar_prefetch=1,
        grid=(rows // BM,),
        in_specs=[
            pl.BlockSpec((BM, d), lambda i, t: (b0 + i, 0)),
            pl.BlockSpec((1, d), lambda i, t: (0, 0)),
            pl.BlockSpec((BM, HEAD), lambda i, t: (b0 + i, 0)),
            pl.BlockSpec((BM, HEAD), lambda i, t: (b0 + i, 0)),
            pl.BlockSpec((d, qw), lambda i, t: (0, 0), pipeline_mode=one),
            pl.BlockSpec((d, kvw), lambda i, t: (0, t[0]), pipeline_mode=one),
            pl.BlockSpec((d, kvw), lambda i, t: (0, t[0]), pipeline_mode=one),
        ] + [ANY] * len(deps),
        out_specs=[
            pl.BlockSpec((BM, qw), lambda i, t: (i, 0)),
            pl.BlockSpec((BM, kvw), lambda i, t: (i, 0)),
            pl.BlockSpec((BM, kvw), lambda i, t: (i, 0)),
        ],
        scratch_shapes=[pltpu.VMEM((BM, d), BF16)],
    )
    return pl.pallas_call(
        _qkv_body, grid_spec=spec, out_shape=[_shape(rows, w) for w in (qw, kvw, kvw)],
        cost_estimate=_cost(2 * rows * d * (qw + 2 * kvw), 2 * rows * d), name="qkv",
    )(t, x, g1, cos, sin, wq, wk, wv, *deps)


def _join(refs, out):
    at = 0
    for r in refs:
        out[at:at + r.shape[0], :] = r[...]
        at += r.shape[0]
    if at < out.shape[0]:
        out[at:, :] = jnp.zeros((out.shape[0] - at, out.shape[1]), out.dtype)


def _attn_body(row0, half, rep, parts, s_ref, q_ref, *refs):
    own_ref, oth_ref, k_ref, v_ref, m_ref, acc_ref = refs[-6:]
    l1 = s_ref[0]
    i = pl.program_id(0)

    @pl.when(i == 0)
    def _():
        _join(refs[:parts], k_ref)
        _join(refs[parts:2 * parts], v_ref)

    nh = half // BQ
    blk = ((i // nh + s_ref[1]) % 2) * nh + i % nh
    q0 = row0 + blk * BQ
    kvl = k_ref.shape[1] // HEAD
    c = HEAD ** -0.5 * 1.4426950408889634
    m_ref[...] = jnp.full_like(m_ref, NEG)
    acc_ref[...] = jnp.zeros_like(acc_ref)
    first = jnp.where(q0 >= l1, l1, 0) // BK
    last = (q0 + BQ - 1) // BK + 1
    ones = jnp.ones((BK, HEAD), BF16)

    def step(j, masked):
        k0 = pl.multiple_of(j * BK, BK)
        if masked:
            row = q0 + lax.broadcasted_iota(jnp.int32, (BQ, BK), 0)
            col = k0 + lax.broadcasted_iota(jnp.int32, (BQ, BK), 1)
            keep = (col <= row) & (col >= jnp.where(row >= l1, l1, 0))
            keep = jnp.concatenate([keep] * rep, axis=0)
        ss = []
        for g in range(kvl):
            q = jnp.concatenate(
                [q_ref[:, (g * rep + r) * HEAD:(g * rep + r + 1) * HEAD] for r in range(rep)], axis=0)
            kk = k_ref[pl.ds(k0, BK), g * HEAD:(g + 1) * HEAD]
            s = lax.dot_general(q, kk, (((1,), (1,)), ((), ())), preferred_element_type=F32)
            ss.append(jnp.where(keep, s, NEG) if masked else s)
        for g in range(kvl):
            s = ss[g]
            m_old = m_ref[g]
            m_new = jnp.maximum(m_old, jnp.max(s, axis=-1, keepdims=True))
            m_ref[g] = m_new
            alpha = jnp.exp2((m_old - m_new) * c)
            p = jnp.exp2((s - m_new[:, :1]) * c).astype(BF16)
            vv = jnp.concatenate([v_ref[pl.ds(k0, BK), g * HEAD:(g + 1) * HEAD], ones], axis=1)
            acc_ref[g] = acc_ref[g] * jnp.concatenate([alpha, alpha], axis=1) + _mm(p, vv)

    def loop(j, carry):
        k0 = j * BK
        one = (q0 >= l1) | (q0 + BQ - 1 < l1)
        clear = (k0 + BK - 1 <= q0) & one & ((q0 < l1) | (k0 >= l1))

        @pl.when(clear)
        def _():
            step(j, False)

        @pl.when(jnp.logical_not(clear))
        def _():
            step(j, True)

        return carry

    lax.fori_loop(first, last, loop, 0)

    def store(o_ref):
        for g in range(kvl):
            o = acc_ref[g, :, :HEAD] / acc_ref[g, :, HEAD:]
            for r in range(rep):
                n = g * rep + r
                o_ref[:, n * HEAD:(n + 1) * HEAD] = o[r * BQ:(r + 1) * BQ].astype(BF16)

    @pl.when(i < nh)
    def _():
        store(own_ref)

    @pl.when(i >= nh)
    def _():
        store(oth_ref)


def _attend(q, k, v, scalars, row0, q_at, rows, rep, deps):
    qw = q.shape[1]
    kvw = k[0].shape[1]
    keys = pl.cdiv(sum(a.shape[0] for a in k), BK) * BK
    half = rows // 2
    nh = half // BQ
    kvl = kvw // HEAD
    qb = q_at // BQ
    spec = pltpu.PrefetchScalarGridSpec(
        num_scalar_prefetch=1,
        grid=(rows // BQ,),
        in_specs=[
            pl.BlockSpec((BQ, qw), lambda i, s: (qb + ((i // nh + s[1]) % 2) * nh + i % nh, 0)),
        ] + [pl.BlockSpec(a.shape, lambda i, s: (0, 0), pipeline_mode=pl.Buffered(1)) for a in k + v]
        + [ANY] * len(deps),
        out_specs=[
            pl.BlockSpec((BQ, qw), lambda i, s: (jnp.minimum(i, nh - 1), 0)),
            pl.BlockSpec((BQ, qw), lambda i, s: (jnp.maximum(i - nh, 0), 0)),
        ],
        scratch_shapes=[
            pltpu.VMEM((keys, kvw), BF16),
            pltpu.VMEM((keys, kvw), BF16),
            pltpu.VMEM((kvl, rep * BQ, HEAD), F32),
            pltpu.VMEM((kvl, rep * BQ, 2 * HEAD), F32),
        ],
    )
    pairs = rows * (row0 + rows // 2) * kvl * rep
    return pl.pallas_call(
        functools.partial(_attn_body, row0, half, rep, len(k)), grid_spec=spec, out_shape=[_shape(half, qw)] * 2,
        cost_estimate=_cost(16 * pairs * HEAD), name="attend",
    )(scalars, q, *k, *v, *deps)


def _proj_body(steps, bn, a_ref, c_ref, w_ref, z_ref, o_ref, oc_ref, buf, sem):
    j = pl.program_id(0)
    kd = w_ref.shape[0]

    def fetch(j):
        slot = j % 3
        at = pl.ds(pl.multiple_of(j * bn, bn), bn)
        return (pltpu.make_async_copy(w_ref.at[:, at], buf.at[slot, :kd], sem.at[slot, 0]),
                pltpu.make_async_copy(z_ref.at[:, at], buf.at[slot, kd:], sem.at[slot, 1]))

    def start(j):
        for c in fetch(j):
            c.start()

    @pl.when(j == 0)
    def _():
        start(0)
        start(1)
        oc_ref[:, :kd] = a_ref[...]
        oc_ref[:, kd:] = c_ref[...]

    @pl.when(j + 2 < steps)
    def _():
        start(j + 2)

    for c in fetch(j):
        c.wait()
    o_ref[...] = _mm(oc_ref[...], buf[j % 3]).astype(BF16)


def _proj(a, c, w, z, bn):
    hr, kd = a.shape
    n = w.shape[1]
    rows = pl.BlockSpec((hr, kd), lambda j: (0, 0), pipeline_mode=pl.Buffered(1))
    return pl.pallas_call(
        functools.partial(_proj_body, n // bn, bn), grid=(n // bn,), in_specs=[rows, rows, ANY, ANY],
        out_specs=pl.BlockSpec((hr, bn), lambda j: (0, j)), out_shape=_shape(hr, n),
        scratch_shapes=[pltpu.VMEM((hr, 2 * kd), BF16), pltpu.VMEM((3, 2 * kd, bn), BF16),
                        pltpu.SemaphoreType.DMA((3, 2))],
        cost_estimate=_cost(4 * hr * kd * n), name="proj",
    )(a, c, w, z)


def _mlp_body(nh, ng, nd, rb, bf, bn, s_ref, x_ref, p_ref, q_ref, g_ref,
              wg_ref, wu_ref, zg_ref, zu_ref, wd_ref, zd_ref, *refs):
    h_ref, o_ref, b_ref, u_ref, gb, ub, db, gsem, usem, dsem = refs[-10:]
    i = pl.program_id(0)
    t = i - nh
    n1 = 2 * ng
    f = ng * bf

    def cols(a, b, j, slot):
        at = pl.ds(pl.multiple_of(j * bf, bf), bf)
        return (pltpu.make_async_copy(a.at[:, at], gb.at[slot], gsem.at[slot]),
                pltpu.make_async_copy(b.at[:, at], ub.at[slot], usem.at[slot]))

    def down(j, slot):
        at = pl.ds(pl.multiple_of(j * bn, bn), bn)
        return (pltpu.make_async_copy(wd_ref.at[:, at], db.at[slot, :f], dsem.at[slot, 0]),
                pltpu.make_async_copy(zd_ref.at[:, at], db.at[slot, f:], dsem.at[slot, 1]))

    def go(copies):
        for c in copies:
            c.start()

    @pl.when(i == 0)
    def _():
        go(cols(wg_ref, wu_ref, 0, 0))

    @pl.when(i < nh)
    def _():
        h = _sum(x_ref[...], _sum(p_ref[...], q_ref[...]))
        h_ref[...] = h
        hf = h.astype(F32)
        ms = jnp.mean(hf * hf, axis=-1, keepdims=True)
        b = (hf * lax.rsqrt(ms + EPS) * g_ref[...].astype(F32)).astype(BF16)
        b_ref[pl.ds(pl.multiple_of(i * rb, rb), rb), :] = b

    @pl.when((t >= 0) & (t < n1))
    def _():
        slot = t % 2

        @pl.when(t + 1 < ng)
        def _():
            go(cols(wg_ref, wu_ref, t + 1, 1 - slot))

        @pl.when((t + 1 >= ng) & (t + 1 < n1))
        def _():
            go(cols(zg_ref, zu_ref, t + 1 - ng, 1 - slot))

        @pl.when(t + 1 == n1)
        def _():
            go(down(0, 0))

        for c in cols(wg_ref, wu_ref, 0, slot):
            c.wait()
        gate = _mm(b_ref[...], gb[slot]).astype(BF16).astype(F32)
        up = _mm(b_ref[...], ub[slot]).astype(BF16).astype(F32)
        u_ref[:, pl.ds(pl.multiple_of(t * bf, bf), bf)] = (jax.nn.silu(gate) * up).astype(BF16)

    @pl.when(t >= n1)
    def _():
        j = t - n1

        @pl.when(j + 1 < nd)
        def _():
            go(down(j + 1, (j + 1) % 2))

        for c in down(j, j % 2):
            c.wait()
        o_ref[...] = _mm(u_ref[...], db[j % 2]).astype(BF16)


def _mlp(x, p, q, g2, scalars, row0, w, z, deps):
    hr, d = p.shape
    f = w[0].shape[1]
    rb, bf, bn = 64, 512, 512
    nh, ng, nd = hr // rb, f // bf, d // bn
    blk = pl.BlockSpec((rb, d), lambda i, s: (jnp.minimum(i, nh - 1), 0))
    return pl.pallas_call(
        functools.partial(_mlp_body, nh, ng, nd, rb, bf, bn),
        grid_spec=pltpu.PrefetchScalarGridSpec(
            num_scalar_prefetch=1, grid=(nh + 2 * ng + nd,),
            in_specs=[pl.BlockSpec((rb, d), lambda i, s: (row0 // rb + s[1] * nh + jnp.minimum(i, nh - 1), 0)),
                      blk, blk, pl.BlockSpec((1, d), lambda i, s: (0, 0))] + [ANY] * (6 + len(deps)),
            out_specs=[blk, pl.BlockSpec((hr, bn), lambda i, s: (0, jnp.maximum(i - nh - 2 * ng, 0)))],
            scratch_shapes=[
                pltpu.VMEM((hr, d), BF16), pltpu.VMEM((hr, 2 * f), BF16),
                pltpu.VMEM((2, d, bf), BF16), pltpu.VMEM((2, d, bf), BF16), pltpu.VMEM((2, 2 * f, bn), BF16),
                pltpu.SemaphoreType.DMA((2,)), pltpu.SemaphoreType.DMA((2,)), pltpu.SemaphoreType.DMA((2, 2))]),
        out_shape=[_shape(hr, d)] * 2,
        compiler_params=pltpu.CompilerParams(vmem_limit_bytes=60 * 1024 * 1024),
        cost_estimate=_cost(12 * hr * d * f), name="mlp",
    )(scalars, x, p, q, g2, w[0], w[1], z[0], z[1], w[2], z[2], *deps)


def _sum(a, b):
    return (a.astype(F32) + b.astype(F32)).astype(BF16)


def _y_body(s_ref, h_ref, p_ref, q_ref, *refs):
    o_ref, y_ref = refs[-2:]
    y = _sum(h_ref[...], _sum(p_ref[...], q_ref[...]))
    o_ref[...] = y
    y_ref[...] = y


def _y(h, p, q, y, n, scalars, row0):
    hr, d = p.shape
    rb = hr // 4
    blk = pl.BlockSpec((rb, d), lambda i, s: (i, 0))
    old = [] if y is None else [y]
    return pl.pallas_call(
        _y_body,
        grid_spec=pltpu.PrefetchScalarGridSpec(
            num_scalar_prefetch=1, grid=(4,), in_specs=[blk, blk, blk] + [ANY] * len(old),
            out_specs=[blk, pl.BlockSpec((rb, d), lambda i, s: (row0 // rb + s[1] * 4 + i, 0))]),
        out_shape=[_shape(hr, d), _shape(n, d)],
        input_output_aliases={} if y is None else {4: 1},
        cost_estimate=_cost(0, 10 * hr * d), name="resid",
    )(scalars, h, p, q, *old)


def _put_body(s_ref, a_ref, y_in, y_ref):
    y_ref[...] = a_ref[...]


def _put(a, y, scalars, row0):
    hr, d = a.shape
    rb = hr // 4
    return pl.pallas_call(
        _put_body,
        grid_spec=pltpu.PrefetchScalarGridSpec(
            num_scalar_prefetch=1, grid=(4,), in_specs=[pl.BlockSpec((rb, d), lambda i, s: (i, 0)), ANY],
            out_specs=pl.BlockSpec((rb, d), lambda i, s: (row0 // rb + (1 - s[1]) * 4 + i, 0))),
        out_shape=_shape(*y.shape), input_output_aliases={2: 0},
        cost_estimate=_cost(0, 4 * hr * d), name="put",
    )(scalars, a, y)


def _cache_body(rb, parts, s_ref, *refs):
    ko_ref, vo_ref, k_ref, v_ref = refs[-4:]
    l1 = s_ref[0]
    n = k_ref.shape[0]
    seg = pl.program_id(0)
    r0 = pl.program_id(1) * rb

    @pl.when((seg == 0) & (r0 == 0))
    def _():
        _join(refs[:parts], k_ref)
        _join(refs[parts:2 * parts], v_ref)

    size = jnp.where(seg == 0, l1, n - l1)
    off = r0 + seg * l1
    at = pl.multiple_of(jnp.minimum(off // 16 * 16, n - rb - 16), 16)
    turn = (2 * (rb + 16) - jnp.minimum(off - at, rb + 16)) % (rb + 16)
    keep = r0 + lax.broadcasted_iota(jnp.int32, (rb, k_ref.shape[1]), 0) < size
    for src, out in ((k_ref, ko_ref), (v_ref, vo_ref)):
        a = pltpu.roll(src[pl.ds(at, rb + 16), :].astype(F32), turn, 0)[:rb]
        out[...] = jnp.where(keep, a, 0.0).astype(BF16)


def _cache(k, v, scalars, n, kvw, deps):
    rb = 512
    out = pl.BlockSpec((rb, kvw), lambda g, i, s: (g * (n // rb) + i, 0))
    return pl.pallas_call(
        functools.partial(_cache_body, rb, len(k)),
        grid_spec=pltpu.PrefetchScalarGridSpec(
            num_scalar_prefetch=1, grid=(2, n // rb),
            in_specs=[pl.BlockSpec(a.shape, lambda g, i, s: (0, 0), pipeline_mode=pl.Buffered(1)) for a in k + v]
            + [ANY] * len(deps),
            out_specs=[out, out],
            scratch_shapes=[pltpu.VMEM((n, kvw), BF16), pltpu.VMEM((n, kvw), BF16)]),
        out_shape=[_shape(2 * n, kvw)] * 2, cost_estimate=_cost(0, 12 * n * kvw), name="cache",
    )(scalars, *k, *v, *deps)


def solution(mesh):
    tp = mesh.shape['tp']
    peer = [(i, i ^ 1) for i in range(tp)]
    across = [(i, i ^ 2) for i in range(tp)]

    def layer(x, lens, g1, g2, wq, wk, wv, wo, wg, wu, wd):
        n, d = x.shape
        t = lax.axis_index('tp')
        core = t % 2
        kvl = wk.shape[1] // HEAD // tp
        kvw = kvl * HEAD
        rep = wq.shape[1] // HEAD // kvl
        l1 = lens[0]
        rows = jnp.arange(n)
        pos = jnp.where(rows >= l1, rows - l1, rows)
        inv = BASE ** (-jnp.arange(0, HEAD, 2, dtype=F32) / HEAD)
        ang = pos.astype(F32)[:, None] * jnp.concatenate([inv, inv])[None, :]
        sign = jnp.where(jnp.arange(HEAD) < HEAD // 2, -1.0, 1.0)[None, :]
        cos = jnp.cos(ang)
        sin = jnp.sin(ang) * sign
        sc = jnp.stack([l1, core]).astype(jnp.int32)
        tv = t.reshape(1).astype(jnp.int32)
        g1r = g1.reshape(1, d)
        g2r = g2.reshape(1, d)
        e = n // 4
        start = [0, e, 2 * e, 3 * e]

        def move(a, perm):
            return lax.ppermute(a, 'tp', perm)

        def qkv(row0, m, *deps):
            return _qkv(x, g1r, cos, sin, wq, wk, wv, tv, row0, m, kvw, deps)

        def att(c, q, q_at, k, v, *deps):
            own, other = _attend(q, k, v, sc, start[c], q_at, e, rep, deps)
            other = move(other, peer)
            return own, other

        def proj(o):
            p = _proj(*o, wo, zo, 640)
            return p, move(p, across)

        def mlp(c, s, *deps):
            h, r = _mlp(x, *s, g2r, sc, start[c], (wg, wu, wd), (zg, zu, zd), deps)
            return h, r, move(r, across)

        def resid(c, r, y):
            own, y = _y(*r, y, n, sc, start[c])
            return y, move(own, peer)

        def put(c, y, other):
            return _put(other, y, sc, start[c])

        zo = move(wo, peer)
        zg = move(wg, peer)
        zu = move(wu, peer)
        zd = move(wd, peer)
        q0, k0, v0 = qkv(0, e)
        p0 = proj(att(0, q0, 0, [k0], [v0]))
        q1, k1, v1 = qkv(e, e, p0[0])
        p1 = proj(att(1, q1, 0, [k0, k1], [v0, v1]))
        q2, k2, v2 = qkv(2 * e, 2 * e, p1[0])
        k, v = [k0, k1, k2], [v0, v1, v2]
        p2 = proj(att(2, q2, 0, k, v))
        p3 = proj(att(3, q2, e, k, v, p2[0]))
        r0 = mlp(0, p0, p3[0])
        r1 = mlp(1, p1, r0[1])
        r2 = mlp(2, p2, r1[1])
        y, other = resid(0, r0, None)
        r3 = mlp(3, p3, r2[1], y)
        y = put(0, y, other)
        for c, r in ((1, r1), (2, r2), (3, r3)):
            y = put(c, *resid(c, r, y))
        kc, vc = _cache(k, v, sc, n, kvw, (r3[1],))
        shape = (2, n, kvl, HEAD)
        return y, kc.reshape(shape), vc.reshape(shape)

    row = P('dp', None)
    cache = P('dp', None, 'tp', None)
    return jax.shard_map(
        layer, mesh=mesh,
        in_specs=(row, P('dp'), P(), P(), P(None, 'tp'), P(), P(), P('tp', None),
                  P(None, 'tp'), P(None, 'tp'), P('tp', None)),
        out_specs=(row, cache, cache), check_vma=False)
```

```python
import functools
import jax
import jax.numpy as jnp
from jax import lax
from jax.experimental import pallas as pl
from jax.experimental.pallas import tpu as pltpu
from jax.sharding import PartitionSpec as P

HEAD = 128
EPS = 1e-5
BASE = 500000.0
BM = 384
BQ = 384
BK = 512
NEG = -0.7 * float(jnp.finfo(jnp.float32).max)
F32 = jnp.float32
BF16 = jnp.bfloat16
ANY = pl.BlockSpec(memory_space=pl.ANY)


def _mm(a, b):
    return jnp.dot(a, b, preferred_element_type=F32)


def _cost(flops=0, nbytes=0):
    return pl.CostEstimate(flops=int(flops + 300 * nbytes), transcendentals=0, bytes_accessed=int(nbytes))


def _shape(*s):
    return jax.ShapeDtypeStruct(s, BF16)


def _qkv_body(t_ref, x_ref, g_ref, cos_ref, sin_ref, wq_ref, wk_ref, wv_ref, *refs):
    q_ref, k_ref, v_ref, a_ref = refs[-4:]
    half = BM // 2
    parts = [pl.ds(z * half, half) for z in range(2)]

    def rope(acc, out, at):
        cos = cos_ref[at, :]
        sin = sin_ref[at, :]
        for h in range(acc.shape[1] // HEAD):
            y = acc[:, h * HEAD:(h + 1) * HEAD]
            out[at, h * HEAD:(h + 1) * HEAD] = (y * cos + pltpu.roll(y, HEAD // 2, 1) * sin).astype(BF16)

    for at in parts:
        xf = x_ref[at, :].astype(F32)
        ms = jnp.mean(xf * xf, axis=-1, keepdims=True)
        a_ref[at, :] = (xf * lax.rsqrt(ms + EPS) * g_ref[...].astype(F32)).astype(BF16)
        rope(_mm(a_ref[at, :], wq_ref[...]), q_ref, at)
        rope(_mm(a_ref[at, :], wk_ref[...]), k_ref, at)
        v_ref[at, :] = _mm(a_ref[at, :], wv_ref[...]).astype(BF16)


def _qkv(x, g1, cos, sin, wq, wk, wv, t, row0, rows, kvw, deps):
    d = x.shape[1]
    qw = wq.shape[1]
    b0 = row0 // BM
    one = pl.Buffered(1)
    spec = pltpu.PrefetchScalarGridSpec(
        num_scalar_prefetch=1,
        grid=(rows // BM,),
        in_specs=[
            pl.BlockSpec((BM, d), lambda i, t: (b0 + i, 0)),
            pl.BlockSpec((1, d), lambda i, t: (0, 0)),
            pl.BlockSpec((BM, HEAD), lambda i, t: (i, 0)),
            pl.BlockSpec((BM, HEAD), lambda i, t: (i, 0)),
            pl.BlockSpec((d, qw), lambda i, t: (0, 0), pipeline_mode=one),
            pl.BlockSpec((d, kvw), lambda i, t: (0, t[0]), pipeline_mode=one),
            pl.BlockSpec((d, kvw), lambda i, t: (0, t[0]), pipeline_mode=one),
        ] + [ANY] * len(deps),
        out_specs=[
            pl.BlockSpec((BM, qw), lambda i, t: (i, 0)),
            pl.BlockSpec((BM, kvw), lambda i, t: (i, 0)),
            pl.BlockSpec((BM, kvw), lambda i, t: (i, 0)),
        ],
        scratch_shapes=[pltpu.VMEM((BM, d), BF16)],
    )
    return pl.pallas_call(
        _qkv_body, grid_spec=spec, out_shape=[_shape(rows, w) for w in (qw, kvw, kvw)],
        cost_estimate=_cost(2 * rows * d * (qw + 2 * kvw), 2 * rows * d), name="qkv",
    )(t, x, g1, cos, sin, wq, wk, wv, *deps)


def _join(refs, out):
    at = 0
    for r in refs:
        out[at:at + r.shape[0], :] = r[...]
        at += r.shape[0]
    if at < out.shape[0]:
        out[at:, :] = jnp.zeros((out.shape[0] - at, out.shape[1]), out.dtype)


def _attn_body(row0, half, rep, parts, s_ref, q_ref, *refs):
    own_ref, oth_ref, k_ref, v_ref, m_ref, acc_ref = refs[-6:]
    l1 = s_ref[0]
    i = pl.program_id(0)

    @pl.when(i == 0)
    def _():
        _join(refs[:parts], k_ref)
        _join(refs[parts:2 * parts], v_ref)

    nh = half // BQ
    blk = ((i // nh + s_ref[1]) % 2) * nh + i % nh
    q0 = row0 + blk * BQ
    kvl = k_ref.shape[1] // HEAD
    c = HEAD ** -0.5 * 1.4426950408889634
    m_ref[...] = jnp.full_like(m_ref, NEG)
    acc_ref[...] = jnp.zeros_like(acc_ref)
    first = jnp.where(q0 >= l1, l1, 0) // BK
    last = (q0 + BQ - 1) // BK + 1
    ones = jnp.ones((BK, HEAD), BF16)

    def step(j, masked):
        k0 = pl.multiple_of(j * BK, BK)
        if masked:
            row = q0 + lax.broadcasted_iota(jnp.int32, (BQ, BK), 0)
            col = k0 + lax.broadcasted_iota(jnp.int32, (BQ, BK), 1)
            keep = (col <= row) & (col >= jnp.where(row >= l1, l1, 0))
            keep = jnp.concatenate([keep] * rep, axis=0)
        ss = []
        for g in range(kvl):
            q = jnp.concatenate(
                [q_ref[:, (g * rep + r) * HEAD:(g * rep + r + 1) * HEAD] for r in range(rep)], axis=0)
            kk = k_ref[pl.ds(k0, BK), g * HEAD:(g + 1) * HEAD]
            s = lax.dot_general(q, kk, (((1,), (1,)), ((), ())), preferred_element_type=F32)
            ss.append(jnp.where(keep, s, NEG) if masked else s)
        for g in range(kvl):
            s = ss[g]
            m_old = m_ref[g]
            m_new = jnp.maximum(m_old, jnp.max(s, axis=-1, keepdims=True))
            m_ref[g] = m_new
            alpha = jnp.exp2((m_old - m_new) * c)
            p = jnp.exp2((s - m_new[:, :1]) * c).astype(BF16)
            vv = jnp.concatenate([v_ref[pl.ds(k0, BK), g * HEAD:(g + 1) * HEAD], ones], axis=1)
            acc_ref[g] = acc_ref[g] * jnp.concatenate([alpha, alpha], axis=1) + _mm(p, vv)

    def loop(j, carry):
        k0 = j * BK
        one = (q0 >= l1) | (q0 + BQ - 1 < l1)
        clear = (k0 + BK - 1 <= q0) & one & ((q0 < l1) | (k0 >= l1))

        @pl.when(clear)
        def _():
            step(j, False)

        @pl.when(jnp.logical_not(clear))
        def _():
            step(j, True)

        return carry

    lax.fori_loop(first, last, loop, 0)

    def store(o_ref):
        for g in range(kvl):
            o = acc_ref[g, :, :HEAD] / acc_ref[g, :, HEAD:]
            for r in range(rep):
                n = g * rep + r
                o_ref[:, n * HEAD:(n + 1) * HEAD] = o[r * BQ:(r + 1) * BQ].astype(BF16)

    @pl.when(i < nh)
    def _():
        store(own_ref)

    @pl.when(i >= nh)
    def _():
        store(oth_ref)


def _attend(q, k, v, scalars, row0, q_at, rows, rep, deps):
    qw = q.shape[1]
    kvw = k[0].shape[1]
    keys = pl.cdiv(sum(a.shape[0] for a in k), BK) * BK
    half = rows // 2
    nh = half // BQ
    kvl = kvw // HEAD
    qb = q_at // BQ
    spec = pltpu.PrefetchScalarGridSpec(
        num_scalar_prefetch=1,
        grid=(rows // BQ,),
        in_specs=[
            pl.BlockSpec((BQ, qw), lambda i, s: (qb + ((i // nh + s[1]) % 2) * nh + i % nh, 0)),
        ] + [pl.BlockSpec(a.shape, lambda i, s: (0, 0), pipeline_mode=pl.Buffered(1)) for a in k + v]
        + [ANY] * len(deps),
        out_specs=[
            pl.BlockSpec((BQ, qw), lambda i, s: (jnp.minimum(i, nh - 1), 0)),
            pl.BlockSpec((BQ, qw), lambda i, s: (jnp.maximum(i - nh, 0), 0)),
        ],
        scratch_shapes=[
            pltpu.VMEM((keys, kvw), BF16),
            pltpu.VMEM((keys, kvw), BF16),
            pltpu.VMEM((kvl, rep * BQ, HEAD), F32),
            pltpu.VMEM((kvl, rep * BQ, 2 * HEAD), F32),
        ],
    )
    pairs = rows * (row0 + rows // 2) * kvl * rep
    return pl.pallas_call(
        functools.partial(_attn_body, row0, half, rep, len(k)), grid_spec=spec, out_shape=[_shape(half, qw)] * 2,
        cost_estimate=_cost(16 * pairs * HEAD), name="attend",
    )(scalars, q, *k, *v, *deps)


def _proj_body(steps, bn, a_ref, c_ref, w_ref, z_ref, o_ref, oc_ref, buf, sem):
    j = pl.program_id(0)
    kd = w_ref.shape[0]

    def fetch(j):
        slot = j % 3
        at = pl.ds(pl.multiple_of(j * bn, bn), bn)
        return (pltpu.make_async_copy(w_ref.at[:, at], buf.at[slot, :kd], sem.at[slot, 0]),
                pltpu.make_async_copy(z_ref.at[:, at], buf.at[slot, kd:], sem.at[slot, 1]))

    def start(j):
        for c in fetch(j):
            c.start()

    @pl.when(j == 0)
    def _():
        start(0)
        start(1)
        oc_ref[:, :kd] = a_ref[...]
        oc_ref[:, kd:] = c_ref[...]

    @pl.when(j + 2 < steps)
    def _():
        start(j + 2)

    for c in fetch(j):
        c.wait()
    o_ref[...] = _mm(oc_ref[...], buf[j % 3]).astype(BF16)


def _proj(a, c, w, z, bn):
    hr, kd = a.shape
    n = w.shape[1]
    rows = pl.BlockSpec((hr, kd), lambda j: (0, 0), pipeline_mode=pl.Buffered(1))
    return pl.pallas_call(
        functools.partial(_proj_body, n // bn, bn), grid=(n // bn,), in_specs=[rows, rows, ANY, ANY],
        out_specs=pl.BlockSpec((hr, bn), lambda j: (0, j)), out_shape=_shape(hr, n),
        scratch_shapes=[pltpu.VMEM((hr, 2 * kd), BF16), pltpu.VMEM((3, 2 * kd, bn), BF16),
                        pltpu.SemaphoreType.DMA((3, 2))],
        cost_estimate=_cost(4 * hr * kd * n), name="proj",
    )(a, c, w, z)


def _mlp_body(nh, ng, nd, rb, bf, bn, s_ref, x_ref, p_ref, q_ref, g_ref,
              wg_ref, wu_ref, zg_ref, zu_ref, wd_ref, zd_ref, *refs):
    h_ref, o_ref, b_ref, u_ref, gb, ub, db, gsem, usem, dsem = refs[-10:]
    i = pl.program_id(0)
    t = i - nh
    n1 = 2 * ng
    f = ng * bf

    def cols(a, b, j, slot):
        at = pl.ds(pl.multiple_of(j * bf, bf), bf)
        return (pltpu.make_async_copy(a.at[:, at], gb.at[slot], gsem.at[slot]),
                pltpu.make_async_copy(b.at[:, at], ub.at[slot], usem.at[slot]))

    def down(j, slot):
        at = pl.ds(pl.multiple_of(j * bn, bn), bn)
        return (pltpu.make_async_copy(wd_ref.at[:, at], db.at[slot, :f], dsem.at[slot, 0]),
                pltpu.make_async_copy(zd_ref.at[:, at], db.at[slot, f:], dsem.at[slot, 1]))

    def go(copies):
        for c in copies:
            c.start()

    @pl.when(i == 0)
    def _():
        go(cols(wg_ref, wu_ref, 0, 0))

    @pl.when(i < nh)
    def _():
        h = _sum(x_ref[...], _sum(p_ref[...], q_ref[...]))
        h_ref[...] = h
        hf = h.astype(F32)
        ms = jnp.mean(hf * hf, axis=-1, keepdims=True)
        b = (hf * lax.rsqrt(ms + EPS) * g_ref[...].astype(F32)).astype(BF16)
        b_ref[pl.ds(pl.multiple_of(i * rb, rb), rb), :] = b

    @pl.when((t >= 0) & (t < n1))
    def _():
        slot = t % 2

        @pl.when(t + 1 < ng)
        def _():
            go(cols(wg_ref, wu_ref, t + 1, 1 - slot))

        @pl.when((t + 1 >= ng) & (t + 1 < n1))
        def _():
            go(cols(zg_ref, zu_ref, t + 1 - ng, 1 - slot))

        @pl.when(t + 1 == n1)
        def _():
            go(down(0, 0))

        for c in cols(wg_ref, wu_ref, 0, slot):
            c.wait()
        half = bf // 2
        for z in range(2):
            gate = _mm(b_ref[...], gb[slot, :, z * half:(z + 1) * half]).astype(BF16).astype(F32)
            up = _mm(b_ref[...], ub[slot, :, z * half:(z + 1) * half]).astype(BF16).astype(F32)
            at = pl.ds(pl.multiple_of(t * bf + z * half, half), half)
            u_ref[:, at] = (jax.nn.silu(gate) * up).astype(BF16)

    @pl.when(t >= n1)
    def _():
        j = t - n1

        @pl.when(j + 1 < nd)
        def _():
            go(down(j + 1, (j + 1) % 2))

        for c in down(j, j % 2):
            c.wait()
        o_ref[...] = _mm(u_ref[...], db[j % 2]).astype(BF16)


def _mlp(x, p, q, g2, scalars, row0, w, z, deps):
    hr, d = p.shape
    f = w[0].shape[1]
    rb, bf, bn = 64, 512, 512
    nh, ng, nd = hr // rb, f // bf, d // bn
    blk = pl.BlockSpec((rb, d), lambda i, s: (jnp.minimum(i, nh - 1), 0))
    return pl.pallas_call(
        functools.partial(_mlp_body, nh, ng, nd, rb, bf, bn),
        grid_spec=pltpu.PrefetchScalarGridSpec(
            num_scalar_prefetch=1, grid=(nh + 2 * ng + nd,),
            in_specs=[pl.BlockSpec((rb, d), lambda i, s: (row0 // rb + s[1] * nh + jnp.minimum(i, nh - 1), 0)),
                      blk, blk, pl.BlockSpec((1, d), lambda i, s: (0, 0))] + [ANY] * (6 + len(deps)),
            out_specs=[blk, pl.BlockSpec((hr, bn), lambda i, s: (0, jnp.maximum(i - nh - 2 * ng, 0)))],
            scratch_shapes=[
                pltpu.VMEM((hr, d), BF16), pltpu.VMEM((hr, 2 * f), BF16),
                pltpu.VMEM((2, d, bf), BF16), pltpu.VMEM((2, d, bf), BF16), pltpu.VMEM((2, 2 * f, bn), BF16),
                pltpu.SemaphoreType.DMA((2,)), pltpu.SemaphoreType.DMA((2,)), pltpu.SemaphoreType.DMA((2, 2))]),
        out_shape=[_shape(hr, d)] * 2,
        compiler_params=pltpu.CompilerParams(vmem_limit_bytes=60 * 1024 * 1024),
        cost_estimate=_cost(12 * hr * d * f), name="mlp",
    )(scalars, x, p, q, g2, w[0], w[1], z[0], z[1], w[2], z[2], *deps)


def _sum(a, b):
    return (a.astype(F32) + b.astype(F32)).astype(BF16)


def _y_body(s_ref, h_ref, p_ref, q_ref, *refs):
    o_ref, y_ref = refs[-2:]
    y = _sum(h_ref[...], _sum(p_ref[...], q_ref[...]))
    o_ref[...] = y
    y_ref[...] = y


def _y(h, p, q, y, n, scalars, row0):
    hr, d = p.shape
    rb = hr // 4
    blk = pl.BlockSpec((rb, d), lambda i, s: (i, 0))
    old = [] if y is None else [y]
    return pl.pallas_call(
        _y_body,
        grid_spec=pltpu.PrefetchScalarGridSpec(
            num_scalar_prefetch=1, grid=(4,), in_specs=[blk, blk, blk] + [ANY] * len(old),
            out_specs=[blk, pl.BlockSpec((rb, d), lambda i, s: (row0 // rb + s[1] * 4 + i, 0))]),
        out_shape=[_shape(hr, d), _shape(n, d)],
        input_output_aliases={} if y is None else {4: 1},
        cost_estimate=_cost(0, 10 * hr * d), name="resid",
    )(scalars, h, p, q, *old)


def _put_body(s_ref, a_ref, y_in, y_ref):
    y_ref[...] = a_ref[...]


def _put(a, y, scalars, row0):
    hr, d = a.shape
    rb = hr // 4
    return pl.pallas_call(
        _put_body,
        grid_spec=pltpu.PrefetchScalarGridSpec(
            num_scalar_prefetch=1, grid=(4,), in_specs=[pl.BlockSpec((rb, d), lambda i, s: (i, 0)), ANY],
            out_specs=pl.BlockSpec((rb, d), lambda i, s: (row0 // rb + (1 - s[1]) * 4 + i, 0))),
        out_shape=_shape(*y.shape), input_output_aliases={2: 0},
        cost_estimate=_cost(0, 4 * hr * d), name="put",
    )(scalars, a, y)


def _cache_body(rb, parts, s_ref, *refs):
    ko_ref, vo_ref, k_ref, v_ref = refs[-4:]
    l1 = s_ref[0]
    n = k_ref.shape[0]
    seg = pl.program_id(0)
    r0 = pl.program_id(1) * rb

    @pl.when((seg == 0) & (r0 == 0))
    def _():
        _join(refs[:parts], k_ref)
        _join(refs[parts:2 * parts], v_ref)

    size = jnp.where(seg == 0, l1, n - l1)
    off = r0 + seg * l1
    at = pl.multiple_of(jnp.minimum(off // 16 * 16, n - rb - 16), 16)
    turn = (2 * (rb + 16) - jnp.minimum(off - at, rb + 16)) % (rb + 16)
    keep = r0 + lax.broadcasted_iota(jnp.int32, (rb, k_ref.shape[1]), 0) < size
    for src, out in ((k_ref, ko_ref), (v_ref, vo_ref)):
        a = pltpu.roll(src[pl.ds(at, rb + 16), :].astype(F32), turn, 0)[:rb]
        out[...] = jnp.where(keep, a, 0.0).astype(BF16)


def _cache(k, v, scalars, n, kvw, deps):
    rb = 512
    out = pl.BlockSpec((rb, kvw), lambda g, i, s: (g * (n // rb) + i, 0))
    return pl.pallas_call(
        functools.partial(_cache_body, rb, len(k)),
        grid_spec=pltpu.PrefetchScalarGridSpec(
            num_scalar_prefetch=1, grid=(2, n // rb),
            in_specs=[pl.BlockSpec(a.shape, lambda g, i, s: (0, 0), pipeline_mode=pl.Buffered(1)) for a in k + v]
            + [ANY] * len(deps),
            out_specs=[out, out],
            scratch_shapes=[pltpu.VMEM((n, kvw), BF16), pltpu.VMEM((n, kvw), BF16)]),
        out_shape=[_shape(2 * n, kvw)] * 2, cost_estimate=_cost(0, 12 * n * kvw), name="cache",
    )(scalars, *k, *v, *deps)


def solution(mesh):
    tp = mesh.shape['tp']
    peer = [(i, i ^ 1) for i in range(tp)]
    across = [(i, i ^ 2) for i in range(tp)]

    def layer(x, lens, g1, g2, wq, wk, wv, wo, wg, wu, wd):
        n, d = x.shape
        t = lax.axis_index('tp')
        core = t % 2
        kvl = wk.shape[1] // HEAD // tp
        kvw = kvl * HEAD
        rep = wq.shape[1] // HEAD // kvl
        l1 = lens[0]
        inv = BASE ** (-jnp.arange(0, HEAD, 2, dtype=F32) / HEAD)
        inv = jnp.concatenate([inv, inv])[None, :]
        sign = jnp.where(jnp.arange(HEAD) < HEAD // 2, -1.0, 1.0)[None, :]

        def angles(l1, row0, m):
            rows = row0 + jnp.arange(m)
            ang = jnp.where(rows >= l1, rows - l1, rows).astype(F32)[:, None] * inv
            return jnp.cos(ang), jnp.sin(ang) * sign

        sc = jnp.stack([l1, core]).astype(jnp.int32)
        tv = t.reshape(1).astype(jnp.int32)
        g1r = g1.reshape(1, d)
        g2r = g2.reshape(1, d)
        e = n // 4
        start = [0, e, 2 * e, 3 * e]

        def move(a, perm):
            return lax.ppermute(a, 'tp', perm)

        def qkv(row0, m, *deps):
            at = lax.optimization_barrier((l1, *deps))[0] if deps else l1
            cos, sin = angles(at, row0, m)
            return _qkv(x, g1r, cos, sin, wq, wk, wv, tv, row0, m, kvw, deps)

        def att(c, q, q_at, k, v, *deps):
            own, other = _attend(q, k, v, sc, start[c], q_at, e, rep, deps)
            other = move(other, peer)
            return own, other

        def proj(o):
            p = _proj(*o, wo, zo, 1024)
            return p, move(p, across)

        def mlp(c, s, *deps):
            h, r = _mlp(x, *s, g2r, sc, start[c], (wg, wu, wd), (zg, zu, zd), deps)
            return h, r, move(r, across)

        def resid(c, r, y):
            own, y = _y(*r, y, n, sc, start[c])
            return y, move(own, peer)

        def put(c, y, other):
            return _put(other, y, sc, start[c])

        zo = move(wo, peer)
        zg = move(wg, peer)
        zu = move(wu, peer)
        zd = move(wd, peer)
        q0, k0, v0 = qkv(0, e)
        p0 = proj(att(0, q0, 0, [k0], [v0]))
        q1, k1, v1 = qkv(e, e, p0[0])
        p1 = proj(att(1, q1, 0, [k0, k1], [v0, v1]))
        q2, k2, v2 = qkv(2 * e, 2 * e, p1[0])
        k, v = [k0, k1, k2], [v0, v1, v2]
        p2 = proj(att(2, q2, 0, k, v))
        p3 = proj(att(3, q2, e, k, v, p2[0]))
        r0 = mlp(0, p0, p3[0])
        r1 = mlp(1, p1, r0[1])
        r2 = mlp(2, p2, r1[1])
        r3 = mlp(3, p3, r2[1])
        y, e0 = resid(0, r0, None)
        y, e1 = resid(1, r1, y)
        y, e2 = resid(2, r2, y)
        for c, other in enumerate((e0, e1, e2)):
            y = put(c, y, other)
        y = put(3, *resid(3, r3, y))
        kc, vc = _cache(k, v, sc, n, kvw, (r3[1],))
        shape = (2, n, kvl, HEAD)
        return y, kc.reshape(shape), vc.reshape(shape)

    row = P('dp', None)
    cache = P('dp', None, 'tp', None)
    return jax.shard_map(
        layer, mesh=mesh,
        in_specs=(row, P('dp'), P(), P(), P(None, 'tp'), P(), P(), P('tp', None),
                  P(None, 'tp'), P(None, 'tp'), P('tp', None)),
        out_specs=(row, cache, cache), check_vma=False)
```
